16 devices in a mesh: dp: 4 (over z, y), dcp: 4 (over x, core).
Axes of the slice: x: 2, y: 2, z: 2, core: 2. Of those that a mesh axis runs over, the one named last changes fastest.
Arguments:
- q_abs: bfloat16 [128, 2, 64, 576], P('dp', None, 'dcp'), parts along dimension 0
- kv_cache: bfloat16 [128, 32, 4, 64, 576], P('dp', None, 'dcp'), parts along dimension 0
- lengths: int32 [128], P('dp'), parts along dimension 0
Outputs:
- output: bfloat16 [128, 2, 64, 512], P('dp', None, 'dcp'), parts along dimension 0
There are 4 independent parts. The reference program is written for one: setup_inputs(seed, part) draws one part's arguments, and reference() takes and returns one part's arrays. A program takes and returns all parts, laid end to end along the dimension named above; each array names one.
All inputs are finite; a program needn't handle non-finite values.
Results may differ from the reference program's by a relative error of at most 0.00786528.
Values are sent between devices in bfloat16 or wider.
A program may use at most 1 GiB of HBM per device.

```python
import math
import jax
import jax.numpy as jnp
from jax import lax

BATCH = 32
MTP = 2
HEADS = 64
LATENT = 512
ROPE = 64
NOPE = 128
ROUNDS = 32
GROUP = 4
PAGE = 64

SEQ = ROUNDS * GROUP * PAGE
WIDTH = LATENT + ROPE


def setup_inputs(seed: int = 0, part: int = 0) -> dict:
    base_key = jax.random.fold_in(jax.random.key(seed), part)
    key_qlat, key_qrope, key_cache, key_len, key_pick = jax.random.split(base_key, 5)
    lat_scale = math.sqrt(SEQ / 256.0)
    q_lat = jax.random.normal(key_qlat, (BATCH, MTP, HEADS, LATENT), jnp.float32) * (math.sqrt(1.8 * (NOPE + ROPE) / LATENT) / lat_scale)
    q_rope = jax.random.normal(key_qrope, (BATCH, MTP, HEADS, ROPE), jnp.float32) * math.sqrt(1.8 * (NOPE + ROPE) / ROPE)
    q_abs = jnp.concatenate([q_lat, q_rope], axis=-1).astype(jnp.bfloat16)
    col_scale = jnp.where(jnp.arange(WIDTH) < LATENT, lat_scale, 1.0)
    kv_cache = (jax.random.normal(key_cache, (BATCH, ROUNDS, GROUP, PAGE, WIDTH), jnp.float32) * col_scale).astype(jnp.bfloat16)
    lengths = jax.random.randint(key_len, (BATCH,), SEQ // 2, SEQ + 1, dtype=jnp.int32)
    longest = jax.random.randint(key_pick, (), 0, BATCH, dtype=jnp.int32)
    lengths = jnp.where(jnp.arange(BATCH) == longest, SEQ, lengths).astype(jnp.int32)
    return {'q_abs': q_abs, 'kv_cache': kv_cache, 'lengths': lengths}


def reference(q_abs, kv_cache, lengths):
    keys_all = kv_cache.reshape(BATCH, SEQ, WIDTH)
    score_scale = (NOPE + ROPE) ** -0.5
    positions = jnp.arange(SEQ)
    offsets = jnp.arange(MTP) - MTP

    def one_seq(seq_args):
        q_seq, key_seq, length = seq_args
        key_f = key_seq.astype(jnp.float32)
        scores = jnp.einsum('thd,sd->ths', q_seq.astype(jnp.float32), key_f) * score_scale
        last_pos = length + offsets
        visible = positions[None, :] <= last_pos[:, None]
        scores = jnp.where(visible[:, None, :], scores, -jnp.inf)
        weights = jax.nn.softmax(scores, axis=-1)
        out_seq = jnp.einsum('ths,sc->thc', weights, key_f[:, :LATENT])
        return out_seq.astype(jnp.bfloat16)

    return lax.map(one_seq, (q_abs, keys_all, lengths))
```

```python
import functools

import jax
import jax.numpy as jnp
from jax import lax
from jax.experimental import pallas as pl
from jax.experimental.pallas import tpu as pltpu
from jax.sharding import PartitionSpec as P

LATENT = 512
ROPE = 64
NOPE = 128
PAGE = 64
BF = jnp.bfloat16
F32 = jnp.float32
MESH = pl.DeviceIdType.MESH

KV_SLOTS = 8
SCALE2 = (NOPE + ROPE) ** -0.5 * 1.4426950408889634
ROWS = 256
NT = (((1,), (1,)), ((), ()))


def kernel(batch, q_hbm, kv_hbm, len_ref, o_ref, kvb, stage, qx, qp, qd, rx, ro, rp, rd, s0, s1, m0, m1, p0, p1,
           ko, so, to, kl, sl, tl, co, cl, cr, cq, fc, fl, kv_sem, st_sem, x_ss, x_rs, f_ss, f_rs, p_ss, p_rs,
           o_ss, o_rs, c_ss, c_rs):
    pairs = batch // 2
    dummy = pairs + 2
    dp = lax.axis_index("dp")
    me = lax.axis_index("dcp")
    core = lax.rem(me, 2)
    peer = me + 1 - 2 * core
    cross = lax.rem(me + 2, 4)
    s_sc, m_sc, p_sc = (s0, s1), (m0, m1), (p0, p1)

    def kv_copy(b):
        slot = lax.rem(b, KV_SLOTS)
        return pltpu.make_async_copy(kv_hbm.at[b, :, 0], kvb.at[slot], kv_sem.at[slot])

    def remote(src, dst, ss, rs, target):
        return pltpu.make_async_remote_copy(src_ref=src, dst_ref=dst, send_sem=ss, recv_sem=rs,
                                            device_id=(dp, target), device_id_type=MESH)

    def piece(k, single):
        return (pl.ds(0, 1) if k == 0 else pl.ds(batch - 1, 1)) if single else pl.ds(2 * k - 1, 2)

    def q_cross(k, single=False):
        r = piece(k, single)
        return (remote(q_hbm.at[r, :, :, 0:LATENT], qx.at[r], x_ss.at[0, k], x_rs.at[0, k], cross),
                remote(ro.at[r], rx.at[r], x_ss.at[1, k], x_rs.at[1, k], cross))

    def q_forward(k, single=False):
        r = piece(k, single)
        return (remote(qx.at[r], qd.at[r], f_ss.at[0, k], f_rs.at[0, k], peer),
                remote(rx.at[r], rd.at[r], f_ss.at[1, k], f_rs.at[1, k], peer))

    def q_peer(k):
        r = pl.ds(0, 1) if k == 0 else pl.ds(1, batch - 1)
        return (remote(q_hbm.at[r, :, :, 0:LATENT], qp.at[r], p_ss.at[0, k], p_rs.at[0, k], peer),
                remote(ro.at[r], rp.at[r], p_ss.at[1, k], p_rs.at[1, k], peer))

    def o_peer(i):
        return (remote(so.at[i], to.at[i], o_ss.at[0, i], o_rs.at[0, i], peer),
                remote(sl.at[i], tl.at[i], o_ss.at[1, i], o_rs.at[1, i], peer))

    def o_cross(i):
        return (remote(co.at[i], cr.at[i], c_ss.at[0, i], c_rs.at[0, i], cross),
                remote(cl.at[i], cq.at[i], c_ss.at[1, i], c_rs.at[1, i], cross))

    stage_first = pltpu.make_async_copy(q_hbm.at[pl.ds(0, 1)], stage.at[pl.ds(0, 1)], st_sem.at[0])
    stage_rest = pltpu.make_async_copy(q_hbm.at[pl.ds(1, batch - 1)], stage.at[pl.ds(1, batch - 1)], st_sem.at[1])
    stage_first.start()
    stage_rest.start()
    for b in range(3):
        kv_copy(b).start()

    barrier = pltpu.get_barrier_semaphore()
    for other in (peer, cross):
        pl.semaphore_signal(barrier, inc=1, device_id=(dp, other), device_id_type=MESH)
    pl.semaphore_wait(barrier, 2)

    q_cross(0, True)[0].start()
    q_peer(0)[0].start()
    q_cross(1)[0].start()
    q_peer(1)[0].start()
    stage_first.wait()

    def pack(b, c):
        both = stage[b, :, :, LATENT:LATENT + ROPE]
        ro[b] = jnp.concatenate([both[0], both[1]], axis=1)
        return c

    pack(0, 0)
    stage_rest.wait()
    q_cross(0, True)[1].start()
    q_peer(0)[1].start()
    lax.fori_loop(1, batch, pack, 0)
    for b in range(3, 5):
        kv_copy(b).start()

    def start_rest(k, c):
        q_cross(k)[0].start()
        q_cross(k)[1].start()
        return c

    q_cross(1)[1].start()
    lax.fori_loop(2, pairs, start_rest, 0)
    for d in q_cross(pairs, True):
        d.start()
    q_peer(1)[1].start()

    lane = lax.broadcasted_iota(jnp.int32, (1, 128), 1)
    token = lax.rem(lane // 16, 2)
    sub = lax.broadcasted_iota(jnp.int32, (PAGE, 1), 0)
    pages = ROWS // PAGE

    def weights(b):
        def cols(lo):
            return jnp.concatenate([r[b, :, :, lo:lo + 256].reshape(32, 256) for r in (stage, qx, qp, qd)], 0)

        qa, qb = cols(0), cols(256)
        packed = [r[b] for r in (ro, rx, rp, rd)]
        qr = jnp.concatenate([x[:, lo:lo + ROPE] for x in packed for lo in (0, ROPE)], 0)
        z = jnp.zeros((128, 256), BF)
        z2 = jnp.zeros((128, ROPE), BF)
        last = jnp.concatenate([jnp.concatenate([qr, z2], 1), jnp.concatenate([z2, qr], 1)], 0)
        return jnp.concatenate([jnp.concatenate([qa, z], 0), jnp.concatenate([qb, z], 0), jnp.concatenate([z, qa], 0),
                                jnp.concatenate([z, qb], 0), last], 1)

    def keys(b, lo):
        slot = lax.rem(b, KV_SLOTS)
        halves = [kvb[slot, f:f + pages].reshape(ROWS, LATENT + ROPE) for f in (lo, lo + 16)]
        return jnp.concatenate([h[:, :LATENT] for h in halves] + [h[:, LATENT:] for h in halves], 1)

    def scores(b, par):
        w = weights(b)
        top = None
        last_pos = len_ref[b] - 2 + token
        for lo in range(0, 16, pages):
            s = lax.dot_general(keys(b, lo), w, NT, preferred_element_type=F32) * SCALE2
            for h in range(2):
                for g in range(pages):
                    t = s[g * PAGE:(g + 1) * PAGE, h * 128:(h + 1) * 128]
                    page = lo + 16 * h + g
                    if page >= 15:
                        pos = (page * 4 + me) * PAGE + sub
                        t = jnp.where(pos <= last_pos, t, -jnp.inf)
                    s_sc[par][page * PAGE:(page + 1) * PAGE, :] = t
                    for r in range(PAGE // 8):
                        v = t[r * 8:(r + 1) * 8]
                        top = v if top is None else jnp.maximum(top, v)
        m_sc[par][...] = top

    def softmax(par):
        m = jnp.max(m_sc[par][...], axis=0, keepdims=True)
        total = None
        for blk in range(16):
            p = jnp.exp2(s_sc[par][blk * 128:(blk + 1) * 128, :] - m)
            for r in range(16):
                v = p[r * 8:(r + 1) * 8]
                total = v if total is None else total + v
            p_sc[par][blk] = p.astype(BF).T
        return m, jnp.sum(total, axis=0, keepdims=True)

    def values(b, par):
        p = jnp.concatenate([p_sc[par][blk] for blk in range(16)], 1)
        v = kvb[lax.rem(b, KV_SLOTS), :, :, 0:LATENT].reshape(2048, LATENT)
        return jnp.dot(p, v, preferred_element_type=F32)

    def finish(i, par, m, total, acc):
        col = jnp.broadcast_to(1.0 / total, (128, 128)).T
        o = (acc * jnp.concatenate([col] * 4, 1)).astype(BF)
        ko[i, par] = o[0:64]
        so[i, par] = o[64:128]
        lse = m + jnp.log2(total)
        kl[i, par:par + 1, :] = lse
        sl[i, par:par + 1, :] = lse

    def combine(i, par):
        l1 = kl[i, par:par + 1, :]
        l2 = tl[i, par:par + 1, :]
        l2 = jnp.concatenate([l2[:, 64:], l2[:, :64]], 1)
        top = jnp.maximum(l1, l2)
        e1, e2 = jnp.exp2(l1 - top), jnp.exp2(l2 - top)
        den = e1 + e2
        w1, w2 = e1 / den, e2 / den
        col = jnp.broadcast_to(jnp.concatenate([w1[:, :64], w2[:, :64]], 1), (128, 128)).T
        c1 = jnp.concatenate([col[:64]] * 4, 1)
        c2 = jnp.concatenate([col[64:]] * 4, 1)
        merged = c1 * ko[i, par].astype(F32) + c2 * to[i, par].astype(F32)
        fc[i, par] = merged[:32]
        co[i, par] = merged[32:].astype(BF)
        lse = top + jnp.log2(den)
        fl[i, par:par + 1, :] = lse
        cl[i, par:par + 1, :] = lse

    for d in q_cross(0, True):
        d.wait_recv()
    for d in q_forward(0, True):
        d.start()
    for d in q_peer(0):
        d.wait_recv()
    kv_copy(0).wait()
    for d in q_forward(0, True):
        d.wait_recv()
    scores(0, 0)
    for d in q_cross(1):
        d.wait_recv()
    for d in q_forward(1):
        d.start()
    for d in q_peer(1):
        d.wait_recv()

    def block(i, final=False):
        a = 2 * i
        done = lax.rem(i + pairs, dummy)
        m, total = softmax(0)
        scores(a + 1, 1)
        finish(i, 0, m, total, values(a, 0))
        combine(done, 0)
        m, total = softmax(1)
        if not final:
            scores(a + 2, 0)
        finish(i, 1, m, total, values(a + 1, 1))
        combine(done, 1)

    def exchange(i):
        @pl.when(i >= 1)
        def _():
            for d in o_peer(i - 1):
                d.start()

        @pl.when(i >= 3)
        def _():
            for d in o_cross(i - 3):
                d.start()

        @pl.when(i >= 2)
        def _():
            for d in o_peer(i - 2):
                d.wait_recv()

    def body(i, c):
        for u in (1, 2):
            kv_copy(2 * i + u).wait()

        @pl.when(2 * i + 6 < batch)
        def _():
            for u in (5, 6):
                kv_copy(2 * i + u).start()

        @pl.when(2 * i + 6 == batch)
        def _():
            kv_copy(batch - 1).start()

        exchange(i)

        @pl.when(i + 2 < pairs)
        def _():
            for d in q_cross(i + 2):
                d.wait_recv()
            for d in q_forward(i + 2):
                d.start()

        @pl.when(i + 2 == pairs)
        def _():
            for d in q_cross(pairs, True):
                d.wait_recv()
            for d in q_forward(pairs, True):
                d.start()

        for d in q_forward(i + 1):
            d.wait_recv()
        block(i)
        return c

    lax.fori_loop(0, pairs - 1, body, 0)
    i = pairs - 1
    kv_copy(batch - 1).wait()
    exchange(i)
    for d in q_forward(pairs, True):
        d.wait_recv()
    block(i, True)
    for d in o_peer(i):
        d.start()
    for d in o_cross(i - 2):
        d.start()
    for j in (i - 1, i):
        for d in o_peer(j):
            d.wait_recv()
        for par in range(2):
            combine(j, par)
        for d in o_cross(j):
            d.start()

    def final(i, c):
        for d in o_cross(i):
            d.wait_recv()
        l1 = fl[i]
        l2 = cq[i]
        l2 = jnp.concatenate([l2[:, 32:], l2[:, :32]], 1)
        top = jnp.maximum(l1, l2)
        e1, e2 = jnp.exp2(l1 - top), jnp.exp2(l2 - top)
        den = e1 + e2
        w1, w2 = e1 / den, e2 / den
        row = jnp.concatenate([w1[0:1, :32], w2[0:1, :32], w1[1:2, :32], w2[1:2, :32]], 1)
        col = jnp.broadcast_to(row, (128, 128)).T
        for par in range(2):
            c1 = jnp.concatenate([col[64 * par:64 * par + 32]] * 4, 1)
            c2 = jnp.concatenate([col[64 * par + 32:64 * par + 64]] * 4, 1)
            o = (c1 * fc[i, par] + c2 * cr[i, par].astype(F32)).astype(BF)
            o_ref[2 * i + par] = o.reshape(2, 16, LATENT)
        return c

    lax.fori_loop(0, pairs, final, 0)

    def drain(k, c):
        for d in (*o_peer(k), *o_cross(k)):
            d.wait_send()
        return c

    lax.fori_loop(0, pairs, drain, 0)

    def drain_q(k, c):
        for d in (*q_cross(k), *q_forward(k)):
            d.wait_send()
        return c

    lax.fori_loop(1, pairs, drain_q, 0)
    for k in (0, pairs):
        for d in (*q_cross(k, True), *q_forward(k, True)):
            d.wait_send()
    for k in range(2):
        for d in q_peer(k):
            d.wait_send()


def solution(mesh):
    def local_step(q_blk, kv_blk, len_blk):
        batch, toks, heads, width = q_blk.shape
        pairs = batch // 2
        n = pairs + 2
        vm = pltpu.VMEM
        q_shape = (batch, toks, heads, LATENT)
        rope_shape = (batch, heads, toks * ROPE)
        dma = pltpu.SemaphoreType.DMA
        return pl.pallas_call(
            functools.partial(kernel, batch),
            out_shape=jax.ShapeDtypeStruct(q_shape, BF),
            in_specs=[pl.BlockSpec(memory_space=pl.ANY), pl.BlockSpec(memory_space=pl.ANY),
                      pl.BlockSpec(memory_space=pltpu.SMEM)],
            out_specs=pl.BlockSpec(memory_space=pltpu.VMEM),
            scratch_shapes=[
                vm((KV_SLOTS, kv_blk.shape[1], PAGE, width), BF),
                vm((batch, toks, heads, width), BF), vm(q_shape, BF), vm(q_shape, BF), vm(q_shape, BF),
                vm(rope_shape, BF), vm(rope_shape, BF), vm(rope_shape, BF), vm(rope_shape, BF),
                vm((2048, 128), F32), vm((2048, 128), F32), vm((8, 128), F32), vm((8, 128), F32),
                vm((16, 128, 128), BF), vm((16, 128, 128), BF),
                vm((n, 2, 64, LATENT), BF), vm((n, 2, 64, LATENT), BF), vm((n, 2, 64, LATENT), BF),
                vm((n, 2, 128), F32), vm((n, 2, 128), F32), vm((n, 2, 128), F32),
                vm((n, 2, 32, LATENT), BF), vm((n, 2, 128), F32), vm((n, 2, 32, LATENT), BF), vm((n, 2, 128), F32),
                vm((n, 2, 32, LATENT), F32), vm((n, 2, 128), F32),
                dma((KV_SLOTS,)), dma((2,)),
                dma((2, pairs + 1)), dma((2, pairs + 1)), dma((2, pairs + 1)), dma((2, pairs + 1)),
                dma((2, 2)), dma((2, 2)),
                dma((2, pairs)), dma((2, pairs)), dma((2, pairs)), dma((2, pairs)),
            ],
            compiler_params=pltpu.CompilerParams(collective_id=0, has_side_effects=True, vmem_limit_bytes=60 << 20),
        )(q_blk, kv_blk, len_blk)

    return jax.shard_map(local_step, mesh=mesh, in_specs=(P('dp', None, 'dcp', None), P('dp', None, 'dcp', None, None), P('dp')),
                         out_specs=P('dp', None, 'dcp', None), check_vma=False)
```

```python
import functools

import jax
import jax.numpy as jnp
from jax import lax
from jax.experimental import pallas as pl
from jax.experimental.pallas import tpu as pltpu
from jax.sharding import PartitionSpec as P

LATENT = 512
ROPE = 64
NOPE = 128
PAGE = 64
BF = jnp.bfloat16
F32 = jnp.float32
MESH = pl.DeviceIdType.MESH

KV_SLOTS = 8
SCALE2 = (NOPE + ROPE) ** -0.5 * 1.4426950408889634
ROWS = 256
NT = (((1,), (1,)), ((), ()))


def kernel(batch, q_hbm, kv_hbm, len_ref, o_ref, kvb, stage, qx, qp, qd, rx, ro, rp, rd, s0, s1, m0, m1, p0, p1,
           ko, so, to, kl, sl, tl, co, cl, cr, cq, fc, fl, kv_sem, st_sem, x_ss, x_rs, f_ss, f_rs, p_ss, p_rs,
           o_ss, o_rs, c_ss, c_rs):
    pairs = batch // 2
    dummy = pairs + 2
    dp = lax.axis_index("dp")
    me = lax.axis_index("dcp")
    core = lax.rem(me, 2)
    peer = me + 1 - 2 * core
    cross = lax.rem(me + 2, 4)
    s_sc, m_sc, p_sc = (s0, s1), (m0, m1), (p0, p1)

    def kv_copy(b):
        slot = lax.rem(b, KV_SLOTS)
        return pltpu.make_async_copy(kv_hbm.at[b, :, 0], kvb.at[slot], kv_sem.at[slot])

    def remote(src, dst, ss, rs, target):
        return pltpu.make_async_remote_copy(src_ref=src, dst_ref=dst, send_sem=ss, recv_sem=rs,
                                            device_id=(dp, target), device_id_type=MESH)

    def piece(k, single):
        return (pl.ds(0, 1) if k == 0 else pl.ds(batch - 1, 1)) if single else pl.ds(2 * k - 1, 2)

    def q_cross(k, single=False):
        r = piece(k, single)
        return (remote((stage if single and k == 0 else q_hbm).at[r, :, :, 0:LATENT], qx.at[r], x_ss.at[0, k], x_rs.at[0, k], cross),
                remote(ro.at[r], rx.at[r], x_ss.at[1, k], x_rs.at[1, k], cross))

    def q_forward(k, single=False):
        r = piece(k, single)
        return (remote(qx.at[r], qd.at[r], f_ss.at[0, k], f_rs.at[0, k], peer),
                remote(rx.at[r], rd.at[r], f_ss.at[1, k], f_rs.at[1, k], peer))

    def q_peer(k):
        r = pl.ds(0, 1) if k == 0 else pl.ds(1, batch - 1)
        return (remote((stage if k == 0 else q_hbm).at[r, :, :, 0:LATENT], qp.at[r], p_ss.at[0, k], p_rs.at[0, k], peer),
                remote(ro.at[r], rp.at[r], p_ss.at[1, k], p_rs.at[1, k], peer))

    def o_peer(i):
        return (remote(so.at[i], to.at[i], o_ss.at[0, i], o_rs.at[0, i], peer),
                remote(sl.at[i], tl.at[i], o_ss.at[1, i], o_rs.at[1, i], peer))

    def o_cross(i):
        return (remote(co.at[i], cr.at[i], c_ss.at[0, i], c_rs.at[0, i], cross),
                remote(cl.at[i], cq.at[i], c_ss.at[1, i], c_rs.at[1, i], cross))

    stage_first = pltpu.make_async_copy(q_hbm.at[pl.ds(0, 1)], stage.at[pl.ds(0, 1)], st_sem.at[0])
    stage_rest = pltpu.make_async_copy(q_hbm.at[pl.ds(1, batch - 1)], stage.at[pl.ds(1, batch - 1)], st_sem.at[1])
    stage_first.start()
    stage_rest.start()

    def pack(b, c):
        both = stage[b, :, :, LATENT:LATENT + ROPE]
        ro[b] = jnp.concatenate([both[0], both[1]], axis=1)
        return c

    barrier = pltpu.get_barrier_semaphore()
    for other in (peer, cross):
        pl.semaphore_signal(barrier, inc=1, device_id=(dp, other), device_id_type=MESH)
    stage_first.wait()
    pack(0, 0)
    pl.semaphore_wait(barrier, 2)

    for d in (*q_cross(0, True), *q_peer(0)):
        d.start()
    q_cross(1)[0].start()
    q_peer(1)[0].start()
    q_cross(2)[0].start()
    for b in range(3):
        kv_copy(b).start()
    stage_rest.wait()
    lax.fori_loop(1, batch, pack, 0)
    q_peer(1)[1].start()
    q_cross(1)[1].start()
    q_cross(2)[1].start()

    def start_rest(k, c):
        for d in q_cross(k):
            d.start()
        return c

    lax.fori_loop(3, pairs, start_rest, 0)
    for d in q_cross(pairs, True):
        d.start()
    for b in range(3, 5):
        kv_copy(b).start()

    lane = lax.broadcasted_iota(jnp.int32, (1, 128), 1)
    token = lax.rem(lane // 16, 2)
    sub = lax.broadcasted_iota(jnp.int32, (PAGE, 1), 0)
    pages = ROWS // PAGE

    def weights(b):
        def cols(lo):
            return jnp.concatenate([r[b, :, :, lo:lo + 256].reshape(32, 256) for r in (stage, qx, qp, qd)], 0)

        qa, qb = cols(0), cols(256)
        packed = [r[b] for r in (ro, rx, rp, rd)]
        qr = jnp.concatenate([x[:, lo:lo + ROPE] for x in packed for lo in (0, ROPE)], 0)
        z = jnp.zeros((128, 256), BF)
        z2 = jnp.zeros((128, ROPE), BF)
        last = jnp.concatenate([jnp.concatenate([qr, z2], 1), jnp.concatenate([z2, qr], 1)], 0)
        return jnp.concatenate([jnp.concatenate([qa, z], 0), jnp.concatenate([qb, z], 0), jnp.concatenate([z, qa], 0),
                                jnp.concatenate([z, qb], 0), last], 1)

    def keys(b, lo):
        slot = lax.rem(b, KV_SLOTS)
        halves = [kvb[slot, f:f + pages].reshape(ROWS, LATENT + ROPE) for f in (lo, lo + 16)]
        return jnp.concatenate([h[:, :LATENT] for h in halves] + [h[:, LATENT:] for h in halves], 1)

    def scores(b, par):
        w = weights(b)
        top = None
        last_pos = len_ref[b] - 2 + token
        for lo in range(0, 16, pages):
            s = lax.dot_general(keys(b, lo), w, NT, preferred_element_type=F32) * SCALE2
            for h in range(2):
                for g in range(pages):
                    t = s[g * PAGE:(g + 1) * PAGE, h * 128:(h + 1) * 128]
                    page = lo + 16 * h + g
                    if page >= 15:
                        pos = (page * 4 + me) * PAGE + sub
                        t = jnp.where(pos <= last_pos, t, -jnp.inf)
                    s_sc[par][page * PAGE:(page + 1) * PAGE, :] = t
                    for r in range(PAGE // 8):
                        v = t[r * 8:(r + 1) * 8]
                        top = v if top is None else jnp.maximum(top, v)
        m_sc[par][...] = top

    def softmax(par):
        m = jnp.max(m_sc[par][...], axis=0, keepdims=True)
        total = None
        for blk in range(16):
            p = jnp.exp2(s_sc[par][blk * 128:(blk + 1) * 128, :] - m)
            for r in range(16):
                v = p[r * 8:(r + 1) * 8]
                total = v if total is None else total + v
            p_sc[par][blk] = p.astype(BF).T
        return m, jnp.sum(total, axis=0, keepdims=True)

    def values(b, par):
        p = jnp.concatenate([p_sc[par][blk] for blk in range(16)], 1)
        v = kvb[lax.rem(b, KV_SLOTS), :, :, 0:LATENT].reshape(2048, LATENT)
        return jnp.dot(p, v, preferred_element_type=F32)

    def finish(i, par, m, total, acc):
        col = jnp.broadcast_to(1.0 / total, (128, 128)).T
        o = (acc * jnp.concatenate([col] * 4, 1)).astype(BF)
        ko[i, par] = o[0:64]
        so[i, par] = o[64:128]
        lse = m + jnp.log2(total)
        kl[i, par:par + 1, :] = lse
        sl[i, par:par + 1, :] = lse

    def combine(i, par):
        l1 = kl[i, par:par + 1, :]
        l2 = tl[i, par:par + 1, :]
        l2 = jnp.concatenate([l2[:, 64:], l2[:, :64]], 1)
        top = jnp.maximum(l1, l2)
        e1, e2 = jnp.exp2(l1 - top), jnp.exp2(l2 - top)
        den = e1 + e2
        w1, w2 = e1 / den, e2 / den
        col = jnp.broadcast_to(jnp.concatenate([w1[:, :64], w2[:, :64]], 1), (128, 128)).T
        c1 = jnp.concatenate([col[:64]] * 4, 1)
        c2 = jnp.concatenate([col[64:]] * 4, 1)
        merged = c1 * ko[i, par].astype(F32) + c2 * to[i, par].astype(F32)
        fc[i, par] = merged[:32]
        co[i, par] = merged[32:].astype(BF)
        lse = top + jnp.log2(den)
        fl[i, par:par + 1, :] = lse
        cl[i, par:par + 1, :] = lse

    for d in q_cross(0, True):
        d.wait_recv()
    for d in q_forward(0, True):
        d.start()
    for d in q_peer(0):
        d.wait_recv()
    kv_copy(0).wait()
    for d in q_forward(0, True):
        d.wait_recv()
    scores(0, 0)
    for d in q_cross(1):
        d.wait_recv()
    for d in q_forward(1):
        d.start()
    for d in q_peer(1):
        d.wait_recv()

    def block(i, final=False):
        a = 2 * i
        done = lax.rem(i + pairs, dummy)
        m, total = softmax(0)
        scores(a + 1, 1)
        finish(i, 0, m, total, values(a, 0))
        combine(done, 0)
        m, total = softmax(1)
        if not final:
            scores(a + 2, 0)
        finish(i, 1, m, total, values(a + 1, 1))
        combine(done, 1)

    def exchange(i):
        @pl.when(i >= 1)
        def _():
            for d in o_peer(i - 1):
                d.start()

        @pl.when(i >= 3)
        def _():
            for d in o_cross(i - 3):
                d.start()

        @pl.when(i >= 2)
        def _():
            for d in o_peer(i - 2):
                d.wait_recv()

    def body(i, c):
        for u in (1, 2):
            kv_copy(2 * i + u).wait()

        @pl.when(2 * i + 6 < batch)
        def _():
            for u in (5, 6):
                kv_copy(2 * i + u).start()

        @pl.when(2 * i + 6 == batch)
        def _():
            kv_copy(batch - 1).start()

        exchange(i)

        @pl.when(i + 2 < pairs)
        def _():
            for d in q_cross(i + 2):
                d.wait_recv()
            for d in q_forward(i + 2):
                d.start()

        @pl.when(i + 2 == pairs)
        def _():
            for d in q_cross(pairs, True):
                d.wait_recv()
            for d in q_forward(pairs, True):
                d.start()

        for d in q_forward(i + 1):
            d.wait_recv()
        block(i)
        return c

    lax.fori_loop(0, pairs - 1, body, 0)
    i = pairs - 1
    kv_copy(batch - 1).wait()
    exchange(i)
    for d in q_forward(pairs, True):
        d.wait_recv()
    block(i, True)
    for d in o_peer(i):
        d.start()
    for d in o_cross(i - 2):
        d.start()
    for j in (i - 1, i):
        for d in o_peer(j):
            d.wait_recv()
        for par in range(2):
            combine(j, par)
        for d in o_cross(j):
            d.start()

    def final(i, c):
        for d in o_cross(i):
            d.wait_recv()
        l1 = fl[i]
        l2 = cq[i]
        l2 = jnp.concatenate([l2[:, 32:], l2[:, :32]], 1)
        top = jnp.maximum(l1, l2)
        e1, e2 = jnp.exp2(l1 - top), jnp.exp2(l2 - top)
        den = e1 + e2
        w1, w2 = e1 / den, e2 / den
        row = jnp.concatenate([w1[0:1, :32], w2[0:1, :32], w1[1:2, :32], w2[1:2, :32]], 1)
        col = jnp.broadcast_to(row, (128, 128)).T
        for par in range(2):
            c1 = jnp.concatenate([col[64 * par:64 * par + 32]] * 4, 1)
            c2 = jnp.concatenate([col[64 * par + 32:64 * par + 64]] * 4, 1)
            o = (c1 * fc[i, par] + c2 * cr[i, par].astype(F32)).astype(BF)
            o_ref[2 * i + par] = o.reshape(2, 16, LATENT)
        return c

    lax.fori_loop(0, pairs, final, 0)

    def drain(k, c):
        for d in (*o_peer(k), *o_cross(k)):
            d.wait_send()
        return c

    lax.fori_loop(0, pairs, drain, 0)

    def drain_q(k, c):
        for d in (*q_cross(k), *q_forward(k)):
            d.wait_send()
        return c

    lax.fori_loop(1, pairs, drain_q, 0)
    for k in (0, pairs):
        for d in (*q_cross(k, True), *q_forward(k, True)):
            d.wait_send()
    for k in range(2):
        for d in q_peer(k):
            d.wait_send()


def solution(mesh):
    def local_step(q_blk, kv_blk, len_blk):
        batch, toks, heads, width = q_blk.shape
        pairs = batch // 2
        n = pairs + 2
        vm = pltpu.VMEM
        q_shape = (batch, toks, heads, LATENT)
        rope_shape = (batch, heads, toks * ROPE)
        dma = pltpu.SemaphoreType.DMA
        return pl.pallas_call(
            functools.partial(kernel, batch),
            out_shape=jax.ShapeDtypeStruct(q_shape, BF),
            in_specs=[pl.BlockSpec(memory_space=pltpu.HBM), pl.BlockSpec(memory_space=pltpu.HBM),
                      pl.BlockSpec(memory_space=pltpu.SMEM)],
            out_specs=pl.BlockSpec(memory_space=pltpu.VMEM),
            scratch_shapes=[
                vm((KV_SLOTS, kv_blk.shape[1], PAGE, width), BF),
                vm((batch, toks, heads, width), BF), vm(q_shape, BF), vm(q_shape, BF), vm(q_shape, BF),
                vm(rope_shape, BF), vm(rope_shape, BF), vm(rope_shape, BF), vm(rope_shape, BF),
                vm((2048, 128), F32), vm((2048, 128), F32), vm((8, 128), F32), vm((8, 128), F32),
                vm((16, 128, 128), BF), vm((16, 128, 128), BF),
                vm((n, 2, 64, LATENT), BF), vm((n, 2, 64, LATENT), BF), vm((n, 2, 64, LATENT), BF),
                vm((n, 2, 128), F32), vm((n, 2, 128), F32), vm((n, 2, 128), F32),
                vm((n, 2, 32, LATENT), BF), vm((n, 2, 128), F32), vm((n, 2, 32, LATENT), BF), vm((n, 2, 128), F32),
                vm((n, 2, 32, LATENT), F32), vm((n, 2, 128), F32),
                dma((KV_SLOTS,)), dma((2,)),
                dma((2, pairs + 1)), dma((2, pairs + 1)), dma((2, pairs + 1)), dma((2, pairs + 1)),
                dma((2, 2)), dma((2, 2)),
                dma((2, pairs)), dma((2, pairs)), dma((2, pairs)), dma((2, pairs)),
            ],
            compiler_params=pltpu.CompilerParams(collective_id=0, has_side_effects=True, vmem_limit_bytes=55_000_000),
        )(q_blk, kv_blk, len_blk)

    return jax.shard_map(local_step, mesh=mesh, in_specs=(P('dp', None, 'dcp', None), P('dp', None, 'dcp', None, None), P('dp')),
                         out_specs=P('dp', None, 'dcp', None), check_vma=False)
```

```python
import functools

import jax
import jax.numpy as jnp
from jax import lax
from jax.experimental import pallas as pl
from jax.experimental.pallas import tpu as pltpu
from jax.sharding import PartitionSpec as P

LATENT = 512
ROPE = 64
NOPE = 128
PAGE = 64
BF = jnp.bfloat16
F32 = jnp.float32
MESH = pl.DeviceIdType.MESH

KV_SLOTS = 8
SCALE2 = (NOPE + ROPE) ** -0.5 * 1.4426950408889634
ROWS = 256
NT = (((1,), (1,)), ((), ()))


def kernel(batch, q_hbm, kv_hbm, len_ref, o_ref, kvb, stage, qx, qp, qd, rx, ro, rp, rd, s0, s1, m0, m1, p0, p1,
           ko, so, to, kl, sl, tl, co, cl, cr, cq, fc, fl, kv_sem, st_sem, x_ss, x_rs, f_ss, f_rs, p_ss, p_rs,
           r_ss, r_rs, o_ss, o_rs, c_ss, c_rs, l_ss, l_rs):
    pairs = batch // 2
    dummy = pairs + 2
    dp = lax.axis_index("dp")
    me = lax.axis_index("dcp")
    core = lax.rem(me, 2)
    peer = me + 1 - 2 * core
    cross = lax.rem(me + 2, 4)
    s_sc, m_sc, p_sc = (s0, s1), (m0, m1), (p0, p1)

    def kv_slot(b):
        return lax.rem(b + 1, KV_SLOTS)

    def kv_copy(k):
        if isinstance(k, int) and k in (0, pairs):
            b = 0 if k == 0 else batch - 1
            slot = kv_slot(b)
            return pltpu.make_async_copy(kv_hbm.at[b, :, 0], kvb.at[slot], kv_sem.at[slot // 2])
        slot = kv_slot(2 * k - 1)
        return pltpu.make_async_copy(kv_hbm.at[pl.ds(2 * k - 1, 2), :, 0], kvb.at[pl.ds(slot, 2)], kv_sem.at[slot // 2])

    def remote(src, dst, ss, rs, target):
        return pltpu.make_async_remote_copy(src_ref=src, dst_ref=dst, send_sem=ss, recv_sem=rs,
                                            device_id=(dp, target), device_id_type=MESH)

    def piece(k, single):
        return (pl.ds(0, 1) if k == 0 else pl.ds(batch - 1, 1)) if single else pl.ds(2 * k - 1, 2)

    def q_cross(k, single=False):
        r = piece(k, single)
        return remote((stage if single and k == 0 else q_hbm).at[r, :, :, 0:LATENT], qx.at[r], x_ss.at[k], x_rs.at[k],
                      cross)

    def q_forward(k, single=False):
        r = piece(k, single)
        return remote(qx.at[r], qd.at[r], f_ss.at[k], f_rs.at[k], peer)

    def q_peer(k):
        r = pl.ds(0, 1) if k == 0 else pl.ds(1, batch - 1)
        return remote((stage if k == 0 else q_hbm).at[r, :, :, 0:LATENT], qp.at[r], p_ss.at[k], p_rs.at[k], peer)

    def rope(k, to_cross, relay):
        r = (pl.ds(0, 1), pl.ds(1, 6), pl.ds(7, batch - 7))[k]
        n = 3 * (0 if to_cross else 2 if relay else 1) + k
        src, dst = (ro, rx) if to_cross else (rx, rd) if relay else (ro, rp)
        return remote(src.at[r], dst.at[r], r_ss.at[n], r_rs.at[n], cross if to_cross else peer)

    def rope_cross(k):
        return rope(k, True, False)

    def rope_peer(k):
        return rope(k, False, False)

    def rope_forward(k):
        return rope(k, False, True)

    def o_peer(i):
        return (remote(so.at[i], to.at[i], o_ss.at[0, i], o_rs.at[0, i], peer),
                remote(sl.at[i], tl.at[i], o_ss.at[1, i], o_rs.at[1, i], peer))

    def o_cross(i):
        return remote(co.at[i], cr.at[i], c_ss.at[i], c_rs.at[i], cross)

    def lse_cross(g):
        return remote(cl.at[2 * g + 1], cq.at[2 * g + 1], l_ss.at[g], l_rs.at[g], cross)

    stage_first = pltpu.make_async_copy(q_hbm.at[pl.ds(0, 1)], stage.at[pl.ds(0, 1)], st_sem.at[0])
    stage_rest = pltpu.make_async_copy(q_hbm.at[pl.ds(1, batch - 1)], stage.at[pl.ds(1, batch - 1)], st_sem.at[1])
    stage_first.start()
    stage_rest.start()

    def pack(b, c):
        both = stage[b, :, :, LATENT:LATENT + ROPE]
        ro[b] = jnp.concatenate([both[0], both[1]], axis=1)
        return c

    barrier = pltpu.get_barrier_semaphore()
    for other in (peer, cross):
        pl.semaphore_signal(barrier, inc=1, device_id=(dp, other), device_id_type=MESH)
    stage_first.wait()
    pack(0, 0)
    pl.semaphore_wait(barrier, 2)

    for d in (q_cross(0, True), rope_cross(0), q_peer(0), rope_peer(0), q_cross(1), q_peer(1)):
        d.start()
    for k in range(2):
        kv_copy(k).start()
    stage_rest.wait()
    lax.fori_loop(1, 7, pack, 0)
    for d in (rope_cross(1), rope_peer(1), q_cross(2), q_cross(3)):
        d.start()
    lax.fori_loop(7, batch, pack, 0)
    for d in (rope_peer(2), rope_cross(2)):
        d.start()

    def start_rest(k, c):
        q_cross(k).start()
        return c

    lax.fori_loop(4, pairs, start_rest, 0)
    q_cross(pairs, True).start()
    kv_copy(2).start()

    lane = lax.broadcasted_iota(jnp.int32, (1, 128), 1)
    token = lax.rem(lane // 16, 2)
    sub = lax.broadcasted_iota(jnp.int32, (PAGE, 1), 0)
    pages = ROWS // PAGE

    def weights(b):
        def cols(lo):
            return jnp.concatenate([r[b, :, :, lo:lo + 256].reshape(32, 256) for r in (stage, qx, qp, qd)], 0)

        qa, qb = cols(0), cols(256)
        packed = [r[b] for r in (ro, rx, rp, rd)]
        qr = jnp.concatenate([x[:, lo:lo + ROPE] for x in packed for lo in (0, ROPE)], 0)
        z = jnp.zeros((128, 256), BF)
        z2 = jnp.zeros((128, ROPE), BF)
        last = jnp.concatenate([jnp.concatenate([qr, z2], 1), jnp.concatenate([z2, qr], 1)], 0)
        return jnp.concatenate([jnp.concatenate([qa, z], 0), jnp.concatenate([qb, z], 0), jnp.concatenate([z, qa], 0),
                                jnp.concatenate([z, qb], 0), last], 1)

    def keys(b, lo):
        slot = kv_slot(b)
        halves = [kvb[slot, f:f + pages].reshape(ROWS, LATENT + ROPE) for f in (lo, lo + 16)]
        return jnp.concatenate([h[:, :LATENT] for h in halves] + [h[:, LATENT:] for h in halves], 1)

    def scores(b, par):
        w = weights(b)
        top = None
        last_pos = len_ref[b] - 2 + token
        for lo in range(0, 16, pages):
            s = lax.dot_general(keys(b, lo), w, NT, preferred_element_type=F32) * SCALE2
            for h in range(2):
                for g in range(pages):
                    t = s[g * PAGE:(g + 1) * PAGE, h * 128:(h + 1) * 128]
                    page = lo + 16 * h + g
                    if page >= 15:
                        pos = (page * 4 + me) * PAGE + sub
                        t = jnp.where(pos <= last_pos, t, -jnp.inf)
                    s_sc[par][page * PAGE:(page + 1) * PAGE, :] = t
                    for r in range(PAGE // 8):
                        v = t[r * 8:(r + 1) * 8]
                        top = v if top is None else jnp.maximum(top, v)
        m_sc[par][...] = top

    def softmax(par):
        m = jnp.max(m_sc[par][...], axis=0, keepdims=True)
        total = None
        for blk in range(16):
            p = jnp.exp2(s_sc[par][blk * 128:(blk + 1) * 128, :] - m)
            for r in range(16):
                v = p[r * 8:(r + 1) * 8]
                total = v if total is None else total + v
            p_sc[par][blk] = p.astype(BF).T
        return m, jnp.sum(total, axis=0, keepdims=True)

    def values(b, par):
        p = jnp.concatenate([p_sc[par][blk] for blk in range(16)], 1)
        v = kvb[kv_slot(b), :, :, 0:LATENT].reshape(2048, LATENT)
        return jnp.dot(p, v, preferred_element_type=F32)

    def finish(i, par, m, total, acc):
        col = jnp.broadcast_to(1.0 / total, (128, 128)).T
        o = (acc * jnp.concatenate([col] * 4, 1)).astype(BF)
        ko[i, par] = o[0:64]
        so[i, par] = o[64:128]
        lse = m + jnp.log2(total)
        kl[i, par:par + 1, :] = lse
        sl[i, par:par + 1, :] = lse

    def combine(i, par):
        l1 = kl[i, par:par + 1, :]
        l2 = tl[i, par:par + 1, :]
        l2 = jnp.concatenate([l2[:, 64:], l2[:, :64]], 1)
        top = jnp.maximum(l1, l2)
        e1, e2 = jnp.exp2(l1 - top), jnp.exp2(l2 - top)
        den = e1 + e2
        w1, w2 = e1 / den, e2 / den
        col = jnp.broadcast_to(jnp.concatenate([w1[:, :64], w2[:, :64]], 1), (128, 128)).T
        c1 = jnp.concatenate([col[:64]] * 4, 1)
        c2 = jnp.concatenate([col[64:]] * 4, 1)
        merged = c1 * ko[i, par].astype(F32) + c2 * to[i, par].astype(F32)
        fc[i, par] = merged[:32]
        co[i, par] = merged[32:].astype(BF)
        lse = top + jnp.log2(den)
        fl[i, par:par + 1, :] = lse
        if par == 1:
            before = lax.rem(i + dummy - 1, dummy)
            cl[i] = jnp.concatenate([r[:, 32:64] for r in (fl[before, 0:1, :], fl[before, 1:2, :], fl[i, 0:1, :], lse)], 1)

    for d in (q_cross(0, True), rope_cross(0)):
        d.wait_recv()
    for d in (q_forward(0, True), rope_forward(0)):
        d.start()
    for d in (q_peer(0), rope_peer(0)):
        d.wait_recv()
    kv_copy(0).wait()
    for d in (q_forward(0, True), rope_forward(0)):
        d.wait_recv()
    scores(0, 0)
    for d in (q_cross(1), rope_cross(1)):
        d.wait_recv()
    for d in (q_forward(1), rope_forward(1)):
        d.start()
    for d in (q_peer(1), rope_peer(1), rope_peer(2)):
        d.wait_recv()
    rope_forward(1).wait_recv()

    def block(i, final=False):
        a = 2 * i
        done = lax.rem(i + pairs, dummy)
        m, total = softmax(0)
        scores(a + 1, 1)
        finish(i, 0, m, total, values(a, 0))
        combine(done, 0)
        m, total = softmax(1)
        if not final:
            scores(a + 2, 0)
        finish(i, 1, m, total, values(a + 1, 1))
        combine(done, 1)

    def step(i):
        static = isinstance(i, int)
        single = static and i + 1 == pairs
        kv_copy(i + 1).wait()
        q_forward(i + 1, single).wait_recv()
        if static and i == 3:
            rope_forward(2).wait_recv()
        if not static or i + 3 <= pairs:
            kv_copy(i + 3).start()
        if not static or i >= 1:
            for d in o_peer(i - 1):
                d.start()
        if not static or i >= 3:
            o_cross(i - 3).start()
            if static and i % 2 == 0:
                lse_cross((i - 4) // 2).start()
            if not static:
                @pl.when(lax.rem(i, 2) == 0)
                def _():
                    lse_cross((i - 4) // 2).start()
        if not static or i + 2 <= pairs:
            single = static and i + 2 == pairs
            q_cross(i + 2, single).wait_recv()
            q_forward(i + 2, single).start()
        if static and i == 2:
            rope_cross(2).wait_recv()
            rope_forward(2).start()
        if not static or i >= 2:
            for d in o_peer(i - 2):
                d.wait_recv()
        block(i, static and i == pairs - 1)

    def body(i, c):
        step(i)
        return c

    for i in range(4):
        step(i)
    lax.fori_loop(4, pairs - 3, body, 0)
    for i in range(pairs - 3, pairs):
        step(i)
    i = pairs - 1
    for d in o_peer(i):
        d.start()
    o_cross(i - 2).start()
    lse_cross((i - 3) // 2).start()
    for j in (i - 1, i):
        for d in o_peer(j):
            d.wait_recv()
        for par in range(2):
            combine(j, par)
        o_cross(j).start()
    lse_cross((i - 1) // 2).start()

    def drain_q(k, c):
        q_cross(k).wait_send()
        q_forward(k).wait_send()
        return c

    lax.fori_loop(1, pairs, drain_q, 0)
    for k in (0, pairs):
        q_cross(k, True).wait_send()
        q_forward(k, True).wait_send()
    for k in range(2):
        q_peer(k).wait_send()
    for k in range(3):
        for d in (rope_cross(k), rope_peer(k), rope_forward(k)):
            d.wait_send()

    def drain_peer(k, c):
        for d in o_peer(k):
            d.wait_send()
        return c

    lax.fori_loop(0, pairs, drain_peer, 0)

    def final(g, c):
        lse_cross(g).wait_recv()
        for u in range(2):
            i = 2 * g + u
            o_cross(i).wait_recv()
            l1 = jnp.concatenate([fl[i, 0:1, :32], fl[i, 1:2, :32]], 1)
            l2 = cq[2 * g + 1][:, 64 * u:64 * u + 64]
            top = jnp.maximum(l1, l2)
            e1, e2 = jnp.exp2(l1 - top), jnp.exp2(l2 - top)
            den = e1 + e2
            col = jnp.broadcast_to(jnp.concatenate([e1 / den, e2 / den], 1), (128, 128)).T
            for par in range(2):
                c1 = jnp.concatenate([col[32 * par:32 * par + 32]] * 4, 1)
                c2 = jnp.concatenate([col[64 + 32 * par:96 + 32 * par]] * 4, 1)
                o = (c1 * fc[i, par] + c2 * cr[i, par].astype(F32)).astype(BF)
                o_ref[2 * i + par] = o.reshape(2, 16, LATENT)
            o_cross(i).wait_send()
        lse_cross(g).wait_send()
        return c

    lax.fori_loop(0, pairs // 2, final, 0)


def solution(mesh):
    def local_step(q_blk, kv_blk, len_blk):
        batch, toks, heads, width = q_blk.shape
        pairs = batch // 2
        n = pairs + 2
        vm = pltpu.VMEM
        q_shape = (batch, toks, heads, LATENT)
        rope_shape = (batch, heads, toks * ROPE)
        dma = pltpu.SemaphoreType.DMA
        return pl.pallas_call(
            functools.partial(kernel, batch),
            out_shape=jax.ShapeDtypeStruct(q_shape, BF),
            in_specs=[pl.BlockSpec(memory_space=pltpu.HBM), pl.BlockSpec(memory_space=pltpu.HBM),
                      pl.BlockSpec(memory_space=pltpu.SMEM)],
            out_specs=pl.BlockSpec(memory_space=pltpu.VMEM),
            scratch_shapes=[
                vm((KV_SLOTS, kv_blk.shape[1], PAGE, width), BF),
                vm((batch, toks, heads, width), BF), vm(q_shape, BF), vm(q_shape, BF), vm(q_shape, BF),
                vm(rope_shape, BF), vm(rope_shape, BF), vm(rope_shape, BF), vm(rope_shape, BF),
                vm((2048, 128), F32), vm((2048, 128), F32), vm((8, 128), F32), vm((8, 128), F32),
                vm((16, 128, 128), BF), vm((16, 128, 128), BF),
                vm((n, 2, 64, LATENT), BF), vm((n, 2, 64, LATENT), BF), vm((n, 2, 64, LATENT), BF),
                vm((n, 2, 128), F32), vm((n, 2, 128), F32), vm((n, 2, 128), F32),
                vm((n, 2, 32, LATENT), BF), vm((n, 1, 128), F32), vm((n, 2, 32, LATENT), BF), vm((n, 1, 128), F32),
                vm((n, 2, 32, LATENT), F32), vm((n, 2, 128), F32),
                dma((KV_SLOTS // 2,)), dma((2,)),
                dma((pairs + 1,)), dma((pairs + 1,)), dma((pairs + 1,)), dma((pairs + 1,)), dma((2,)), dma((2,)),
                dma((9,)), dma((9,)), dma((2, pairs)), dma((2, pairs)), dma((pairs,)), dma((pairs,)),
                dma((pairs // 2,)), dma((pairs // 2,)),
            ],
            compiler_params=pltpu.CompilerParams(collective_id=0, has_side_effects=True, vmem_limit_bytes=55_000_000),
        )(q_blk, kv_blk, len_blk)

    return jax.shard_map(local_step, mesh=mesh, in_specs=(P('dp', None, 'dcp', None), P('dp', None, 'dcp', None, None), P('dp')),
                         out_specs=P('dp', None, 'dcp', None), check_vma=False)
```

```python
import functools

import jax
import jax.numpy as jnp
from jax import lax
from jax.experimental import pallas as pl
from jax.experimental.pallas import tpu as pltpu
from jax.sharding import PartitionSpec as P

LATENT = 512
ROPE = 64
NOPE = 128
PAGE = 64
BF = jnp.bfloat16
F32 = jnp.float32
MESH = pl.DeviceIdType.MESH

KV_SLOTS = 8
SCALE2 = (NOPE + ROPE) ** -0.5 * 1.4426950408889634
ROWS = 256
NT = (((1,), (1,)), ((), ()))


def kernel(batch, q_hbm, kv_hbm, len_hbm, o_ref, len_ref, kvb, stage, qx, qp, qd, rx, ro, rp, rd, s0, s1, m0, m1, p0, p1,
           ko, so, to, kl, sl, tl, co, cl, cr, cq, fc, fl, kv_sem, st_sem, x_ss, x_rs, f_ss, f_rs, p_ss, p_rs,
           r_ss, r_rs, o_ss, o_rs, c_ss, c_rs, l_ss, l_rs):
    pairs = batch // 2
    dummy = pairs + 2
    dp = lax.axis_index("dp")
    me = lax.axis_index("dcp")
    core = lax.rem(me, 2)
    peer = me + 1 - 2 * core
    cross = lax.rem(me + 2, 4)
    s_sc, m_sc, p_sc = (s0, s1), (m0, m1), (p0, p1)

    def kv_slot(b):
        return lax.rem(b + 1, KV_SLOTS)

    def kv_copy(k):
        if isinstance(k, int) and k in (0, pairs):
            b = 0 if k == 0 else batch - 1
            slot = kv_slot(b)
            return pltpu.make_async_copy(kv_hbm.at[b, :, 0], kvb.at[slot], kv_sem.at[slot // 2])
        slot = kv_slot(2 * k - 1)
        return pltpu.make_async_copy(kv_hbm.at[pl.ds(2 * k - 1, 2), :, 0], kvb.at[pl.ds(slot, 2)], kv_sem.at[slot // 2])

    def remote(src, dst, ss, rs, target):
        return pltpu.make_async_remote_copy(src_ref=src, dst_ref=dst, send_sem=ss, recv_sem=rs,
                                            device_id=(dp, target), device_id_type=MESH)

    def piece(k, single):
        return (pl.ds(0, 1) if k == 0 else pl.ds(batch - 1, 1)) if single else pl.ds(2 * k - 1, 2)

    def q_cross(k, single=False):
        r = piece(k, single)
        return remote(q_hbm.at[r, :, :, 0:LATENT], qx.at[r], x_ss.at[k], x_rs.at[k],
                      cross)

    def q_forward(k, single=False):
        r = piece(k, single)
        return remote(qx.at[r], qd.at[r], f_ss.at[k], f_rs.at[k], peer)

    def q_peer(k):
        r = pl.ds(0, 1) if k == 0 else pl.ds(1, batch - 1)
        return remote(q_hbm.at[r, :, :, 0:LATENT], qp.at[r], p_ss.at[k], p_rs.at[k], peer)

    def rope(k, to_cross, relay):
        r = (pl.ds(0, 1), pl.ds(1, 6), pl.ds(7, batch - 7))[k]
        n = 3 * (0 if to_cross else 2 if relay else 1) + k
        src, dst = (ro, rx) if to_cross else (rx, rd) if relay else (ro, rp)
        return remote(src.at[r], dst.at[r], r_ss.at[n], r_rs.at[n], cross if to_cross else peer)

    def rope_cross(k):
        return rope(k, True, False)

    def rope_peer(k):
        return rope(k, False, False)

    def rope_forward(k):
        return rope(k, False, True)

    def o_peer(i):
        return (remote(so.at[i], to.at[i], o_ss.at[0, i], o_rs.at[0, i], peer),
                remote(sl.at[i], tl.at[i], o_ss.at[1, i], o_rs.at[1, i], peer))

    def o_cross(i):
        return remote(co.at[i], cr.at[i], c_ss.at[i], c_rs.at[i], cross)

    def lse_cross(g):
        return remote(cl.at[2 * g + 1], cq.at[2 * g + 1], l_ss.at[g], l_rs.at[g], cross)

    stage_first = pltpu.make_async_copy(q_hbm.at[pl.ds(0, 1)], stage.at[pl.ds(0, 1)], st_sem.at[0])
    stage_rest = pltpu.make_async_copy(q_hbm.at[pl.ds(1, batch - 1)], stage.at[pl.ds(1, batch - 1)], st_sem.at[1])
    stage_first.start()
    stage_rest.start()
    len_copy = pltpu.make_async_copy(len_hbm, len_ref, st_sem.at[2])
    len_copy.start()

    def pack(b, c):
        both = stage[b, :, :, LATENT:LATENT + ROPE]
        ro[b] = jnp.concatenate([both[0], both[1]], axis=1)
        return c

    barrier = pltpu.get_barrier_semaphore()
    for other in (peer, cross):
        pl.semaphore_signal(barrier, inc=1, device_id=(dp, other), device_id_type=MESH)
    pl.semaphore_wait(barrier, 2)

    for d in (q_cross(0, True), q_peer(0)):
        d.start()
    stage_first.wait()
    pack(0, 0)
    for d in (rope_cross(0), rope_peer(0), q_cross(1), q_peer(1)):
        d.start()
    for k in range(2):
        kv_copy(k).start()
    stage_rest.wait()
    lax.fori_loop(1, 7, pack, 0)
    for d in (rope_cross(1), rope_peer(1), q_cross(2), q_cross(3)):
        d.start()
    lax.fori_loop(7, batch, pack, 0)
    for d in (rope_peer(2), rope_cross(2)):
        d.start()

    def start_rest(k, c):
        q_cross(k).start()
        return c

    lax.fori_loop(4, pairs, start_rest, 0)
    q_cross(pairs, True).start()
    kv_copy(2).start()

    lane = lax.broadcasted_iota(jnp.int32, (1, 128), 1)
    token = lax.rem(lane // 16, 2)
    sub = lax.broadcasted_iota(jnp.int32, (PAGE, 1), 0)
    pages = ROWS // PAGE

    def weights(b):
        def cols(lo):
            return jnp.concatenate([r[b, :, :, lo:lo + 256].reshape(32, 256) for r in (stage, qx, qp, qd)], 0)

        qa, qb = cols(0), cols(256)
        packed = [r[b] for r in (ro, rx, rp, rd)]
        qr = jnp.concatenate([x[:, lo:lo + ROPE] for x in packed for lo in (0, ROPE)], 0)
        z = jnp.zeros((128, 256), BF)
        z2 = jnp.zeros((128, ROPE), BF)
        last = jnp.concatenate([jnp.concatenate([qr, z2], 1), jnp.concatenate([z2, qr], 1)], 0)
        return jnp.concatenate([jnp.concatenate([qa, z], 0), jnp.concatenate([qb, z], 0), jnp.concatenate([z, qa], 0),
                                jnp.concatenate([z, qb], 0), last], 1)

    def keys(b, lo):
        slot = kv_slot(b)
        halves = [kvb[slot, f:f + pages].reshape(ROWS, LATENT + ROPE) for f in (lo, lo + 16)]
        return jnp.concatenate([h[:, :LATENT] for h in halves] + [h[:, LATENT:] for h in halves], 1)

    def scores(b, par):
        w = weights(b)
        top = None
        last_pos = len_ref[b] - 2 + token
        for lo in range(0, 16, pages):
            s = lax.dot_general(keys(b, lo), w, NT, preferred_element_type=F32) * SCALE2
            for h in range(2):
                for g in range(pages):
                    t = s[g * PAGE:(g + 1) * PAGE, h * 128:(h + 1) * 128]
                    page = lo + 16 * h + g
                    if page >= 15:
                        pos = (page * 4 + me) * PAGE + sub
                        t = jnp.where(pos <= last_pos, t, -jnp.inf)
                    s_sc[par][page * PAGE:(page + 1) * PAGE, :] = t
                    for r in range(PAGE // 8):
                        v = t[r * 8:(r + 1) * 8]
                        top = v if top is None else jnp.maximum(top, v)
        m_sc[par][...] = top

    def softmax(par):
        m = jnp.max(m_sc[par][...], axis=0, keepdims=True)
        total = None
        for blk in range(16):
            p = jnp.exp2(s_sc[par][blk * 128:(blk + 1) * 128, :] - m)
            for r in range(16):
                v = p[r * 8:(r + 1) * 8]
                total = v if total is None else total + v
            p_sc[par][blk] = p.astype(BF).T
        return m, jnp.sum(total, axis=0, keepdims=True)

    def values(b, par):
        p = jnp.concatenate([p_sc[par][blk] for blk in range(16)], 1)
        v = kvb[kv_slot(b), :, :, 0:LATENT].reshape(2048, LATENT)
        return jnp.dot(p, v, preferred_element_type=F32)

    def finish(i, par, m, total, acc):
        col = jnp.broadcast_to(1.0 / total, (128, 128)).T
        o = (acc * jnp.concatenate([col] * 4, 1)).astype(BF)
        ko[i, par] = o[0:64]
        so[i, par] = o[64:128]
        lse = m + jnp.log2(total)
        kl[i, par:par + 1, :] = lse
        sl[i, par:par + 1, :] = lse

    def combine(i, par):
        l1 = kl[i, par:par + 1, :]
        l2 = tl[i, par:par + 1, :]
        l2 = jnp.concatenate([l2[:, 64:], l2[:, :64]], 1)
        top = jnp.maximum(l1, l2)
        e1, e2 = jnp.exp2(l1 - top), jnp.exp2(l2 - top)
        den = e1 + e2
        w1, w2 = e1 / den, e2 / den
        col = jnp.broadcast_to(jnp.concatenate([w1[:, :64], w2[:, :64]], 1), (128, 128)).T
        c1 = jnp.concatenate([col[:64]] * 4, 1)
        c2 = jnp.concatenate([col[64:]] * 4, 1)
        merged = c1 * ko[i, par].astype(F32) + c2 * to[i, par].astype(F32)
        fc[i, par] = merged[:32]
        co[i, par] = merged[32:].astype(BF)
        lse = top + jnp.log2(den)
        fl[i, par:par + 1, :] = lse
        if par == 1:
            before = lax.rem(i + dummy - 1, dummy)
            cl[i] = jnp.concatenate([r[:, 32:64] for r in (fl[before, 0:1, :], fl[before, 1:2, :], fl[i, 0:1, :], lse)], 1)

    for d in (q_cross(0, True), rope_cross(0)):
        d.wait_recv()
    for d in (q_forward(0, True), rope_forward(0)):
        d.start()
    for d in (q_peer(0), rope_peer(0)):
        d.wait_recv()
    kv_copy(0).wait()
    len_copy.wait()
    for d in (q_forward(0, True), rope_forward(0)):
        d.wait_recv()
    scores(0, 0)
    for d in (q_cross(1), rope_cross(1)):
        d.wait_recv()
    for d in (q_forward(1), rope_forward(1)):
        d.start()
    for d in (q_peer(1), rope_peer(1), rope_peer(2)):
        d.wait_recv()
    rope_forward(1).wait_recv()

    def block(i, final=False):
        a = 2 * i
        done = lax.rem(i + pairs, dummy)
        m, total = softmax(0)
        scores(a + 1, 1)
        finish(i, 0, m, total, values(a, 0))
        combine(done, 0)
        m, total = softmax(1)
        if not final:
            scores(a + 2, 0)
        finish(i, 1, m, total, values(a + 1, 1))
        combine(done, 1)

    def step(i):
        static = isinstance(i, int)
        single = static and i + 1 == pairs
        kv_copy(i + 1).wait()
        q_forward(i + 1, single).wait_recv()
        if static and i == 3:
            rope_forward(2).wait_recv()
        if not static or i + 3 <= pairs:
            kv_copy(i + 3).start()
        if not static or i >= 1:
            for d in o_peer(i - 1):
                d.start()
        if not static or i >= 3:
            o_cross(i - 3).start()
            if static and i % 2 == 0:
                lse_cross((i - 4) // 2).start()
            if not static:
                @pl.when(lax.rem(i, 2) == 0)
                def _():
                    lse_cross((i - 4) // 2).start()
        if not static or i + 2 <= pairs:
            single = static and i + 2 == pairs
            q_cross(i + 2, single).wait_recv()
            q_forward(i + 2, single).start()
        if static and i == 2:
            rope_cross(2).wait_recv()
            rope_forward(2).start()
        if not static or i >= 2:
            for d in o_peer(i - 2):
                d.wait_recv()
        block(i, static and i == pairs - 1)

    def body(i, c):
        step(i)
        return c

    for i in range(4):
        step(i)
    lax.fori_loop(4, pairs - 3, body, 0)
    for i in range(pairs - 3, pairs):
        step(i)
    i = pairs - 1
    for d in o_peer(i):
        d.start()
    o_cross(i - 2).start()
    lse_cross((i - 3) // 2).start()
    for j in (i - 1, i):
        for d in o_peer(j):
            d.wait_recv()
        for par in range(2):
            combine(j, par)
        o_cross(j).start()
    lse_cross((i - 1) // 2).start()

    def drain_q(k, c):
        q_cross(k).wait_send()
        q_forward(k).wait_send()
        return c

    lax.fori_loop(1, pairs, drain_q, 0)
    for k in (0, pairs):
        q_cross(k, True).wait_send()
        q_forward(k, True).wait_send()
    for k in range(2):
        q_peer(k).wait_send()
    for k in range(3):
        for d in (rope_cross(k), rope_peer(k), rope_forward(k)):
            d.wait_send()

    def drain_peer(k, c):
        for d in o_peer(k):
            d.wait_send()
        return c

    lax.fori_loop(0, pairs, drain_peer, 0)

    def final(g, c):
        lse_cross(g).wait_recv()
        for u in range(2):
            i = 2 * g + u
            o_cross(i).wait_recv()
            l1 = jnp.concatenate([fl[i, 0:1, :32], fl[i, 1:2, :32]], 1)
            l2 = cq[2 * g + 1][:, 64 * u:64 * u + 64]
            top = jnp.maximum(l1, l2)
            e1, e2 = jnp.exp2(l1 - top), jnp.exp2(l2 - top)
            den = e1 + e2
            col = jnp.broadcast_to(jnp.concatenate([e1 / den, e2 / den], 1), (128, 128)).T
            for par in range(2):
                c1 = jnp.concatenate([col[32 * par:32 * par + 32]] * 4, 1)
                c2 = jnp.concatenate([col[64 + 32 * par:96 + 32 * par]] * 4, 1)
                o = (c1 * fc[i, par] + c2 * cr[i, par].astype(F32)).astype(BF)
                o_ref[2 * i + par] = o.reshape(2, 16, LATENT)
            o_cross(i).wait_send()
        lse_cross(g).wait_send()
        return c

    lax.fori_loop(0, pairs // 2, final, 0)


def solution(mesh):
    def local_step(q_blk, kv_blk, len_blk):
        batch, toks, heads, width = q_blk.shape
        pairs = batch // 2
        n = pairs + 2
        vm = pltpu.VMEM
        q_shape = (batch, toks, heads, LATENT)
        rope_shape = (batch, heads, toks * ROPE)
        dma = pltpu.SemaphoreType.DMA
        return pl.pallas_call(
            functools.partial(kernel, batch),
            out_shape=jax.ShapeDtypeStruct(q_shape, BF),
            in_specs=[pl.BlockSpec(memory_space=pltpu.HBM), pl.BlockSpec(memory_space=pltpu.HBM),
                      pl.BlockSpec(memory_space=pltpu.HBM)],
            out_specs=pl.BlockSpec(memory_space=pltpu.VMEM),
            scratch_shapes=[
                pltpu.SMEM((batch,), jnp.int32),
                vm((KV_SLOTS, kv_blk.shape[1], PAGE, width), BF),
                vm((batch, toks, heads, width), BF), vm(q_shape, BF), vm(q_shape, BF), vm(q_shape, BF),
                vm(rope_shape, BF), vm(rope_shape, BF), vm(rope_shape, BF), vm(rope_shape, BF),
                vm((2048, 128), F32), vm((2048, 128), F32), vm((8, 128), F32), vm((8, 128), F32),
                vm((16, 128, 128), BF), vm((16, 128, 128), BF),
                vm((n, 2, 64, LATENT), BF), vm((n, 2, 64, LATENT), BF), vm((n, 2, 64, LATENT), BF),
                vm((n, 2, 128), F32), vm((n, 2, 128), F32), vm((n, 2, 128), F32),
                vm((n, 2, 32, LATENT), BF), vm((n, 1, 128), F32), vm((n, 2, 32, LATENT), BF), vm((n, 1, 128), F32),
                vm((n, 2, 32, LATENT), F32), vm((n, 2, 128), F32),
                dma((KV_SLOTS // 2,)), dma((3,)),
                dma((pairs + 1,)), dma((pairs + 1,)), dma((pairs + 1,)), dma((pairs + 1,)), dma((2,)), dma((2,)),
                dma((9,)), dma((9,)), dma((2, pairs)), dma((2, pairs)), dma((pairs,)), dma((pairs,)),
                dma((pairs // 2,)), dma((pairs // 2,)),
            ],
            compiler_params=pltpu.CompilerParams(collective_id=0, has_side_effects=True, vmem_limit_bytes=55_000_000),
        )(*(pltpu.with_memory_space_constraint(x, pltpu.HBM) for x in (q_blk, kv_blk, len_blk)))

    return jax.shard_map(local_step, mesh=mesh, in_specs=(P('dp', None, 'dcp', None), P('dp', None, 'dcp', None, None), P('dp')),
                         out_specs=P('dp', None, 'dcp', None), check_vma=False)
```

```python
import functools

import jax
import jax.numpy as jnp
from jax import lax
from jax.experimental import pallas as pl
from jax.experimental.pallas import tpu as pltpu
from jax.sharding import PartitionSpec as P

LATENT = 512
ROPE = 64
NOPE = 128
PAGE = 64
BF = jnp.bfloat16
F32 = jnp.float32
MESH = pl.DeviceIdType.MESH

KV_SLOTS = 8
SCALE2 = (NOPE + ROPE) ** -0.5 * 1.4426950408889634
ROWS = 256
NT = (((1,), (1,)), ((), ()))


def kernel(batch, q_hbm, kv_hbm, len_hbm, o_ref, len_ref, kvb, stage, qx, qp, qd, rx, ro, rp, rd, s0, s1, m0, m1, p0, p1,
           ko, so, to, kl, sl, tl, co, cl, cr, cq, fc, fl, kv_sem, st_sem, x_ss, x_rs, f_ss, f_rs, p_ss, p_rs,
           r_ss, r_rs, o_ss, o_rs, c_ss, c_rs, l_ss, l_rs):
    pairs = batch // 2
    dummy = pairs + 2
    dp = lax.axis_index("dp")
    me = lax.axis_index("dcp")
    core = lax.rem(me, 2)
    peer = me + 1 - 2 * core
    cross = lax.rem(me + 2, 4)
    s_sc, m_sc, p_sc = (s0, s1), (m0, m1), (p0, p1)

    def kv_slot(b):
        return lax.rem(b + 1, KV_SLOTS)

    def kv_copy(k):
        if isinstance(k, int) and k in (0, pairs):
            b = 0 if k == 0 else batch - 1
            slot = kv_slot(b)
            return pltpu.make_async_copy(kv_hbm.at[b, :, 0], kvb.at[slot], kv_sem.at[slot // 2])
        slot = kv_slot(2 * k - 1)
        return pltpu.make_async_copy(kv_hbm.at[pl.ds(2 * k - 1, 2), :, 0], kvb.at[pl.ds(slot, 2)], kv_sem.at[slot // 2])

    def remote(src, dst, ss, rs, target):
        return pltpu.make_async_remote_copy(src_ref=src, dst_ref=dst, send_sem=ss, recv_sem=rs,
                                            device_id=(dp, target), device_id_type=MESH)

    def piece(k, single):
        return (pl.ds(0, 1) if k == 0 else pl.ds(batch - 1, 1)) if single else pl.ds(2 * k - 1, 2)

    def q_cross(k, single=False):
        r = piece(k, single)
        return remote(q_hbm.at[r, :, :, 0:LATENT], qx.at[r], x_ss.at[k], x_rs.at[k],
                      cross)

    def q_forward(k, single=False):
        r = piece(k, single)
        return remote(qx.at[r], qd.at[r], f_ss.at[k], f_rs.at[k], peer)

    def q_peer(k):
        r = pl.ds(0, 1) if k == 0 else pl.ds(1, batch - 1)
        return remote(q_hbm.at[r, :, :, 0:LATENT], qp.at[r], p_ss.at[k], p_rs.at[k], peer)

    def rope(k, to_cross, relay):
        r = (pl.ds(0, 1), pl.ds(1, 6), pl.ds(7, batch - 7))[k]
        n = 3 * (0 if to_cross else 2 if relay else 1) + k
        src, dst = (ro, rx) if to_cross else (rx, rd) if relay else (ro, rp)
        return remote(src.at[r], dst.at[r], r_ss.at[n], r_rs.at[n], cross if to_cross else peer)

    def rope_cross(k):
        return rope(k, True, False)

    def rope_peer(k):
        return rope(k, False, False)

    def rope_forward(k):
        return rope(k, False, True)

    def o_peer(i):
        return (remote(so.at[i], to.at[i], o_ss.at[0, i], o_rs.at[0, i], peer),
                remote(sl.at[i], tl.at[i], o_ss.at[1, i], o_rs.at[1, i], peer))

    def o_cross(i):
        return remote(co.at[i], cr.at[i], c_ss.at[i], c_rs.at[i], cross)

    def lse_cross(g):
        return remote(cl.at[2 * g + 1], cq.at[2 * g + 1], l_ss.at[g], l_rs.at[g], cross)

    stage_first = pltpu.make_async_copy(q_hbm.at[pl.ds(0, 1)], stage.at[pl.ds(0, 1)], st_sem.at[0])
    stage_rest = pltpu.make_async_copy(q_hbm.at[pl.ds(1, batch - 1)], stage.at[pl.ds(1, batch - 1)], st_sem.at[1])
    stage_first.start()
    stage_rest.start()
    len_copy = pltpu.make_async_copy(len_hbm, len_ref, st_sem.at[2])
    len_copy.start()

    def pack(b, c):
        both = stage[b, :, :, LATENT:LATENT + ROPE]
        ro[b] = jnp.concatenate([both[0], both[1]], axis=1)
        return c

    barrier = pltpu.get_barrier_semaphore()
    for other in (peer, cross):
        pl.semaphore_signal(barrier, inc=1, device_id=(dp, other), device_id_type=MESH)
    pl.semaphore_wait(barrier, 2)

    for d in (q_cross(0, True), q_peer(0)):
        d.start()
    stage_first.wait()
    pack(0, 0)
    for d in (rope_cross(0), rope_peer(0), q_cross(1), q_peer(1)):
        d.start()
    for k in range(2):
        kv_copy(k).start()
    stage_rest.wait()
    lax.fori_loop(1, 7, pack, 0)
    for d in (rope_cross(1), rope_peer(1), q_cross(2), q_cross(3)):
        d.start()
    lax.fori_loop(7, batch, pack, 0)
    for d in (rope_peer(2), rope_cross(2)):
        d.start()

    def start_rest(k, c):
        q_cross(k).start()
        return c

    lax.fori_loop(4, pairs, start_rest, 0)
    q_cross(pairs, True).start()
    kv_copy(2).start()

    lane = lax.broadcasted_iota(jnp.int32, (1, 128), 1)
    token = lax.rem(lane // 16, 2)
    sub = lax.broadcasted_iota(jnp.int32, (PAGE, 1), 0)
    pages = ROWS // PAGE

    def weights(b):
        def cols(lo):
            return jnp.concatenate([r[b, :, :, lo:lo + 256].reshape(32, 256) for r in (stage, qx, qp, qd)], 0)

        qa, qb = cols(0), cols(256)
        packed = [r[b] for r in (ro, rx, rp, rd)]
        qr = jnp.concatenate([x[:, lo:lo + ROPE] for x in packed for lo in (0, ROPE)], 0)
        z = jnp.zeros((128, 256), BF)
        z2 = jnp.zeros((128, ROPE), BF)
        last = jnp.concatenate([jnp.concatenate([qr, z2], 1), jnp.concatenate([z2, qr], 1)], 0)
        return jnp.concatenate([jnp.concatenate([qa, z], 0), jnp.concatenate([qb, z], 0), jnp.concatenate([z, qa], 0),
                                jnp.concatenate([z, qb], 0), last], 1)

    def keys(b, lo):
        slot = kv_slot(b)
        halves = [kvb[slot, f:f + pages].reshape(ROWS, LATENT + ROPE) for f in (lo, lo + 16)]
        return jnp.concatenate([h[:, :LATENT] for h in halves] + [h[:, LATENT:] for h in halves], 1)

    def scores(b, par):
        w = weights(b)
        top = None
        last_pos = len_ref[b] - 2 + token
        for lo in range(0, 16, pages):
            s = lax.dot_general(keys(b, lo), w, NT, preferred_element_type=F32) * SCALE2
            for h in range(2):
                for g in range(pages):
                    t = s[g * PAGE:(g + 1) * PAGE, h * 128:(h + 1) * 128]
                    page = lo + 16 * h + g
                    if page >= 15:
                        pos = (page * 4 + me) * PAGE + sub
                        t = jnp.where(pos <= last_pos, t, -jnp.inf)
                    s_sc[par][page * PAGE:(page + 1) * PAGE, :] = t
                    for r in range(PAGE // 8):
                        v = t[r * 8:(r + 1) * 8]
                        top = v if top is None else jnp.maximum(top, v)
        m_sc[par][...] = top

    def softmax(par):
        m = jnp.max(m_sc[par][...], axis=0, keepdims=True)
        total = None
        for blk in range(16):
            p = jnp.exp2(s_sc[par][blk * 128:(blk + 1) * 128, :] - m)
            for r in range(16):
                v = p[r * 8:(r + 1) * 8]
                total = v if total is None else total + v
            p_sc[par][blk] = p.astype(BF).T
        return m, jnp.sum(total, axis=0, keepdims=True)

    def values(b, par):
        p = jnp.concatenate([p_sc[par][blk] for blk in range(16)], 1)
        v = kvb[kv_slot(b), :, :, 0:LATENT].reshape(2048, LATENT)
        return jnp.dot(p, v, preferred_element_type=F32)

    def finish(i, par, m, total, acc):
        col = jnp.broadcast_to(1.0 / total, (128, 128)).T
        o = (acc * jnp.concatenate([col] * 4, 1)).astype(BF)
        ko[i, par] = o[0:64]
        so[i, par] = o[64:128]
        lse = m + jnp.log2(total)
        kl[i, par:par + 1, :] = lse
        sl[i, par:par + 1, :] = lse

    def combine(i, par):
        l1 = kl[i, par:par + 1, :]
        l2 = tl[i, par:par + 1, :]
        l2 = jnp.concatenate([l2[:, 64:], l2[:, :64]], 1)
        top = jnp.maximum(l1, l2)
        e1, e2 = jnp.exp2(l1 - top), jnp.exp2(l2 - top)
        den = e1 + e2
        w1, w2 = e1 / den, e2 / den
        col = jnp.broadcast_to(jnp.concatenate([w1[:, :64], w2[:, :64]], 1), (128, 128)).T
        c1 = jnp.concatenate([col[:64]] * 4, 1)
        c2 = jnp.concatenate([col[64:]] * 4, 1)
        merged = c1 * ko[i, par].astype(F32) + c2 * to[i, par].astype(F32)
        fc[i, par] = merged[:32]
        co[i, par] = merged[32:].astype(BF)
        lse = top + jnp.log2(den)
        fl[i, par:par + 1, :] = lse
        if par == 1:
            before = lax.rem(i + dummy - 1, dummy)
            cl[i] = jnp.concatenate([r[:, 32:64] for r in (fl[before, 0:1, :], fl[before, 1:2, :], fl[i, 0:1, :], lse)], 1)

    for d in (q_cross(0, True), rope_cross(0)):
        d.wait_recv()
    for d in (q_forward(0, True), rope_forward(0)):
        d.start()
    for d in (q_peer(0), rope_peer(0)):
        d.wait_recv()
    kv_copy(0).wait()
    len_copy.wait()
    for d in (q_forward(0, True), rope_forward(0)):
        d.wait_recv()
    scores(0, 0)
    for d in (q_cross(1), rope_cross(1)):
        d.wait_recv()
    for d in (q_forward(1), rope_forward(1)):
        d.start()
    for d in (q_peer(1), rope_peer(1), rope_peer(2)):
        d.wait_recv()
    rope_forward(1).wait_recv()

    def block(i, final=False):
        a = 2 * i
        done = lax.rem(i + pairs, dummy)
        m, total = softmax(0)
        scores(a + 1, 1)
        finish(i, 0, m, total, values(a, 0))
        combine(done, 0)
        m, total = softmax(1)
        if not final:
            scores(a + 2, 0)
        finish(i, 1, m, total, values(a + 1, 1))
        combine(done, 1)

    def step(i):
        static = isinstance(i, int)
        single = static and i + 1 == pairs
        kv_copy(i + 1).wait()
        q_forward(i + 1, single).wait_recv()
        if static and i == 3:
            rope_forward(2).wait_recv()
        if not static or i + 3 <= pairs:
            kv_copy(i + 3).start()
        if not static or i >= 1:
            for d in o_peer(i - 1):
                d.start()
        if not static or i >= 3:
            if static and i % 2 == 0:
                lse_cross((i - 4) // 2).start()
            if not static:
                @pl.when(lax.rem(i, 2) == 0)
                def _():
                    lse_cross((i - 4) // 2).start()
            o_cross(i - 3).start()
        if not static or i + 2 <= pairs:
            single = static and i + 2 == pairs
            q_cross(i + 2, single).wait_recv()
            q_forward(i + 2, single).start()
        if static and i == 2:
            rope_cross(2).wait_recv()
            rope_forward(2).start()
        if not static or i >= 2:
            for d in o_peer(i - 2):
                d.wait_recv()
        block(i, static and i == pairs - 1)

    def body(i, c):
        step(i)
        return c

    for i in range(4):
        step(i)
    lax.fori_loop(4, pairs - 3, body, 0)
    for i in range(pairs - 3, pairs):
        step(i)
    i = pairs - 1
    for d in o_peer(i):
        d.start()
    lse_cross((i - 3) // 2).start()
    o_cross(i - 2).start()
    for j in (i - 1, i):
        for d in o_peer(j):
            d.wait_recv()
        for par in range(2):
            combine(j, par)
        if j == i:
            lse_cross((i - 1) // 2).start()
        o_cross(j).start()

    def drain_q(k, c):
        q_cross(k).wait_send()
        q_forward(k).wait_send()
        return c

    lax.fori_loop(1, pairs, drain_q, 0)
    for k in (0, pairs):
        q_cross(k, True).wait_send()
        q_forward(k, True).wait_send()
    for k in range(2):
        q_peer(k).wait_send()
    for k in range(3):
        for d in (rope_cross(k), rope_peer(k), rope_forward(k)):
            d.wait_send()

    def drain_peer(k, c):
        for d in o_peer(k):
            d.wait_send()
        return c

    lax.fori_loop(0, pairs, drain_peer, 0)

    def final(g, c):
        lse_cross(g).wait_recv()
        cols = []
        for u in range(2):
            i = 2 * g + u
            l1 = jnp.concatenate([fl[i, 0:1, :32], fl[i, 1:2, :32]], 1)
            l2 = cq[2 * g + 1][:, 64 * u:64 * u + 64]
            top = jnp.maximum(l1, l2)
            e1, e2 = jnp.exp2(l1 - top), jnp.exp2(l2 - top)
            den = e1 + e2
            col = jnp.broadcast_to(jnp.concatenate([e1 / den, e2 / den], 1), (128, 128)).T
            for par in range(2):
                fc[i, par] = fc[i, par] * jnp.concatenate([col[32 * par:32 * par + 32]] * 4, 1)
            cols.append(col[64:])
        for u in range(2):
            i = 2 * g + u
            o_cross(i).wait_recv()
            for par in range(2):
                c2 = jnp.concatenate([cols[u][32 * par:32 * par + 32]] * 4, 1)
                o_ref[2 * i + par] = (fc[i, par] + c2 * cr[i, par].astype(F32)).astype(BF).reshape(2, 16, LATENT)
        for u in range(2):
            o_cross(2 * g + u).wait_send()
        lse_cross(g).wait_send()
        return c

    lax.fori_loop(0, pairs // 2, final, 0)


def solution(mesh):
    def local_step(q_blk, kv_blk, len_blk):
        batch, toks, heads, width = q_blk.shape
        pairs = batch // 2
        n = pairs + 2
        vm = pltpu.VMEM
        q_shape = (batch, toks, heads, LATENT)
        rope_shape = (batch, heads, toks * ROPE)
        dma = pltpu.SemaphoreType.DMA
        return pl.pallas_call(
            functools.partial(kernel, batch),
            out_shape=jax.ShapeDtypeStruct(q_shape, BF),
            in_specs=[pl.BlockSpec(memory_space=pltpu.HBM), pl.BlockSpec(memory_space=pltpu.HBM),
                      pl.BlockSpec(memory_space=pltpu.HBM)],
            out_specs=pl.BlockSpec(memory_space=pltpu.VMEM),
            scratch_shapes=[
                pltpu.SMEM((batch,), jnp.int32),
                vm((KV_SLOTS, kv_blk.shape[1], PAGE, width), BF),
                vm((batch, toks, heads, width), BF), vm(q_shape, BF), vm(q_shape, BF), vm(q_shape, BF),
                vm(rope_shape, BF), vm(rope_shape, BF), vm(rope_shape, BF), vm(rope_shape, BF),
                vm((2048, 128), F32), vm((2048, 128), F32), vm((8, 128), F32), vm((8, 128), F32),
                vm((16, 128, 128), BF), vm((16, 128, 128), BF),
                vm((n, 2, 64, LATENT), BF), vm((n, 2, 64, LATENT), BF), vm((n, 2, 64, LATENT), BF),
                vm((n, 2, 128), F32), vm((n, 2, 128), F32), vm((n, 2, 128), F32),
                vm((n, 2, 32, LATENT), BF), vm((n, 1, 128), F32), vm((n, 2, 32, LATENT), BF), vm((n, 1, 128), F32),
                vm((n, 2, 32, LATENT), F32), vm((n, 2, 128), F32),
                dma((KV_SLOTS // 2,)), dma((3,)),
                dma((pairs + 1,)), dma((pairs + 1,)), dma((pairs + 1,)), dma((pairs + 1,)), dma((2,)), dma((2,)),
                dma((9,)), dma((9,)), dma((2, pairs)), dma((2, pairs)), dma((pairs,)), dma((pairs,)),
                dma((pairs // 2,)), dma((pairs // 2,)),
            ],
            compiler_params=pltpu.CompilerParams(collective_id=0, has_side_effects=True, vmem_limit_bytes=55_000_000),
        )(*(pltpu.with_memory_space_constraint(x, pltpu.HBM) for x in (q_blk, kv_blk, len_blk)))

    return jax.shard_map(local_step, mesh=mesh, in_specs=(P('dp', None, 'dcp', None), P('dp', None, 'dcp', None, None), P('dp')),
                         out_specs=P('dp', None, 'dcp', None), check_vma=False)
```

```python
import functools

import jax
import jax.numpy as jnp
from jax import lax
from jax.experimental import pallas as pl
from jax.experimental.pallas import tpu as pltpu
from jax.sharding import PartitionSpec as P

LATENT = 512
ROPE = 64
NOPE = 128
PAGE = 64
BF = jnp.bfloat16
F32 = jnp.float32
MESH = pl.DeviceIdType.MESH

KV_SLOTS = 8
SCALE2 = (NOPE + ROPE) ** -0.5 * 1.4426950408889634
ROWS = 256
NT = (((1,), (1,)), ((), ()))


def kernel(batch, q_hbm, kv_hbm, len_hbm, o_ref, len_ref, kvb, stage, qx, qp, qd, rx, ro, rp, rd, s0, s1, m0, m1, p0, p1,
           ko, so, to, kl, sl, tl, co, cl, cr, cq, fc, fl, kv_sem, st_sem, x_ss, x_rs, f_ss, f_rs, p_ss, p_rs,
           r_ss, r_rs, o_ss, o_rs, c_ss, c_rs, l_ss, l_rs):
    pairs = batch // 2
    dummy = pairs + 2
    dp = lax.axis_index("dp")
    me = lax.axis_index("dcp")
    core = lax.rem(me, 2)
    peer = me + 1 - 2 * core
    cross = lax.rem(me + 2, 4)
    s_sc, m_sc, p_sc = (s0, s1), (m0, m1), (p0, p1)

    def kv_slot(b):
        return lax.rem(b + 1, KV_SLOTS)

    def kv_copy(k):
        if isinstance(k, int) and k in (0, pairs):
            b = 0 if k == 0 else batch - 1
            slot = kv_slot(b)
            return pltpu.make_async_copy(kv_hbm.at[b, :, 0], kvb.at[slot], kv_sem.at[slot // 2])
        slot = kv_slot(2 * k - 1)
        return pltpu.make_async_copy(kv_hbm.at[pl.ds(2 * k - 1, 2), :, 0], kvb.at[pl.ds(slot, 2)], kv_sem.at[slot // 2])

    def remote(src, dst, ss, rs, target):
        return pltpu.make_async_remote_copy(src_ref=src, dst_ref=dst, send_sem=ss, recv_sem=rs,
                                            device_id=(dp, target), device_id_type=MESH)

    def piece(k, single):
        return (pl.ds(0, 1) if k == 0 else pl.ds(batch - 1, 1)) if single else pl.ds(2 * k - 1, 2)

    def q_cross(k, single=False):
        r = piece(k, single)
        return remote(q_hbm.at[r, :, :, 0:LATENT], qx.at[r], x_ss.at[k], x_rs.at[k],
                      cross)

    def q_forward(k, single=False):
        r = piece(k, single)
        return remote(qx.at[r], qd.at[r], f_ss.at[k], f_rs.at[k], peer)

    def q_peer(k):
        r = pl.ds(0, 1) if k == 0 else pl.ds(1, batch - 1)
        return remote(q_hbm.at[r, :, :, 0:LATENT], qp.at[r], p_ss.at[k], p_rs.at[k], peer)

    def rope(k, to_cross, relay):
        r = (pl.ds(0, 1), pl.ds(1, 6), pl.ds(7, batch - 7))[k]
        n = 3 * (0 if to_cross else 2 if relay else 1) + k
        src, dst = (ro, rx) if to_cross else (rx, rd) if relay else (ro, rp)
        return remote(src.at[r], dst.at[r], r_ss.at[n], r_rs.at[n], cross if to_cross else peer)

    def rope_cross(k):
        return rope(k, True, False)

    def rope_peer(k):
        return rope(k, False, False)

    def rope_forward(k):
        return rope(k, False, True)

    def o_peer(i):
        return (remote(so.at[i], to.at[i], o_ss.at[0, i], o_rs.at[0, i], peer),
                remote(sl.at[i], tl.at[i], o_ss.at[1, i], o_rs.at[1, i], peer))

    whole = pairs // 2 - 2

    def o_cross(k):
        r = pl.ds(whole + k, 1) if isinstance(k, int) and k >= whole else pl.ds(2 * k, 2)
        return remote(co.at[r], cr.at[r], c_ss.at[k], c_rs.at[k], cross)

    def lse_cross(k):
        r = pl.ds(whole // 2 + k, 1) if isinstance(k, int) and k >= whole // 2 else pl.ds(2 * k, 2)
        return remote(cl.at[r], cq.at[r], l_ss.at[k], l_rs.at[k], cross)

    barrier = pltpu.get_barrier_semaphore()
    for other in (cross, peer):
        pl.semaphore_signal(barrier, inc=1, device_id=(dp, other), device_id_type=MESH)

    stage_first = pltpu.make_async_copy(q_hbm.at[pl.ds(0, 1)], stage.at[pl.ds(0, 1)], st_sem.at[0])
    stage_rest = pltpu.make_async_copy(q_hbm.at[pl.ds(1, batch - 1)], stage.at[pl.ds(1, batch - 1)], st_sem.at[1])
    stage_first.start()
    stage_rest.start()
    len_copy = pltpu.make_async_copy(len_hbm, len_ref, st_sem.at[2])
    len_copy.start()

    def pack(b, c):
        both = stage[b, :, :, LATENT:LATENT + ROPE]
        ro[b] = jnp.concatenate([both[0], both[1]], axis=1)
        return c

    pl.semaphore_wait(barrier, 2)

    for d in (q_cross(0, True), q_peer(0)):
        d.start()
    stage_first.wait()
    pack(0, 0)
    for d in (rope_cross(0), rope_peer(0), q_cross(1), q_peer(1)):
        d.start()
    for k in range(2):
        kv_copy(k).start()
    stage_rest.wait()
    lax.fori_loop(1, 7, pack, 0)
    for d in (rope_cross(1), rope_peer(1), q_cross(2), q_cross(3)):
        d.start()
    lax.fori_loop(7, batch, pack, 0)
    for d in (rope_peer(2), rope_cross(2)):
        d.start()

    def start_rest(k, c):
        q_cross(k).start()
        return c

    lax.fori_loop(4, pairs, start_rest, 0)
    q_cross(pairs, True).start()
    kv_copy(2).start()

    lane = lax.broadcasted_iota(jnp.int32, (1, 128), 1)
    token = lax.rem(lane // 16, 2)
    sub = lax.broadcasted_iota(jnp.int32, (PAGE, 1), 0)
    pages = ROWS // PAGE

    def weights(b):
        def cols(lo):
            return jnp.concatenate([r[b, :, :, lo:lo + 256].reshape(32, 256) for r in (stage, qx, qp, qd)], 0)

        qa, qb = cols(0), cols(256)
        packed = [r[b] for r in (ro, rx, rp, rd)]
        qr = jnp.concatenate([x[:, lo:lo + ROPE] for x in packed for lo in (0, ROPE)], 0)
        z = jnp.zeros((128, 256), BF)
        z2 = jnp.zeros((128, ROPE), BF)
        last = jnp.concatenate([jnp.concatenate([qr, z2], 1), jnp.concatenate([z2, qr], 1)], 0)
        return jnp.concatenate([jnp.concatenate([qa, z], 0), jnp.concatenate([qb, z], 0), jnp.concatenate([z, qa], 0),
                                jnp.concatenate([z, qb], 0), last], 1)

    def keys(b, lo):
        slot = kv_slot(b)
        halves = [kvb[slot, f:f + pages].reshape(ROWS, LATENT + ROPE) for f in (lo, lo + 16)]
        return jnp.concatenate([h[:, :LATENT] for h in halves] + [h[:, LATENT:] for h in halves], 1)

    def scores(b, par):
        w = weights(b)
        top = None
        last_pos = len_ref[b] - 2 + token
        for lo in range(0, 16, pages):
            s = lax.dot_general(keys(b, lo), w, NT, preferred_element_type=F32) * SCALE2
            for h in range(2):
                for g in range(pages):
                    t = s[g * PAGE:(g + 1) * PAGE, h * 128:(h + 1) * 128]
                    page = lo + 16 * h + g
                    if page >= 15:
                        pos = (page * 4 + me) * PAGE + sub
                        t = jnp.where(pos <= last_pos, t, -jnp.inf)
                    s_sc[par][page * PAGE:(page + 1) * PAGE, :] = t
                    for r in range(PAGE // 8):
                        v = t[r * 8:(r + 1) * 8]
                        top = v if top is None else jnp.maximum(top, v)
        m_sc[par][...] = top

    def softmax(par):
        m = jnp.max(m_sc[par][...], axis=0, keepdims=True)
        total = None
        for blk in range(16):
            p = jnp.exp2(s_sc[par][blk * 128:(blk + 1) * 128, :] - m)
            for r in range(16):
                v = p[r * 8:(r + 1) * 8]
                total = v if total is None else total + v
            p_sc[par][blk] = p.astype(BF).T
        return m, jnp.sum(total, axis=0, keepdims=True)

    def values(b, par):
        p = jnp.concatenate([p_sc[par][blk] for blk in range(16)], 1)
        v = kvb[kv_slot(b), :, :, 0:LATENT].reshape(2048, LATENT)
        return jnp.dot(p, v, preferred_element_type=F32)

    def finish(i, par, m, total, acc):
        col = jnp.broadcast_to(1.0 / total, (128, 128)).T
        o = (acc * jnp.concatenate([col] * 4, 1)).astype(BF)
        ko[i, par] = o[0:64]
        so[i, par] = o[64:128]
        lse = m + jnp.log2(total)
        kl[i, par:par + 1, :] = lse
        sl[i, par:par + 1, :] = lse

    def combine(i, par):
        l1 = kl[i, par:par + 1, :]
        l2 = tl[i, par:par + 1, :]
        l2 = jnp.concatenate([l2[:, 64:], l2[:, :64]], 1)
        top = jnp.maximum(l1, l2)
        e1, e2 = jnp.exp2(l1 - top), jnp.exp2(l2 - top)
        den = e1 + e2
        w1, w2 = e1 / den, e2 / den
        col = jnp.broadcast_to(jnp.concatenate([w1[:, :64], w2[:, :64]], 1), (128, 128)).T
        c1 = jnp.concatenate([col[:64]] * 4, 1)
        c2 = jnp.concatenate([col[64:]] * 4, 1)
        merged = c1 * ko[i, par].astype(F32) + c2 * to[i, par].astype(F32)
        fc[i, par] = merged[:32]
        co[i, par] = merged[32:].astype(BF)
        lse = top + jnp.log2(den)
        fl[i, par:par + 1, :] = lse
        if par == 1:
            before = lax.rem(i + dummy - 1, dummy)
            cl[i // 2] = jnp.concatenate([r[:, 32:64] for r in (fl[before, 0:1, :], fl[before, 1:2, :], fl[i, 0:1, :], lse)], 1)

    for d in (q_cross(0, True), rope_cross(0)):
        d.wait_recv()
    for d in (q_forward(0, True), rope_forward(0)):
        d.start()
    for d in (q_peer(0), rope_peer(0)):
        d.wait_recv()
    kv_copy(0).wait()
    len_copy.wait()
    for d in (q_forward(0, True), rope_forward(0)):
        d.wait_recv()
    scores(0, 0)
    for d in (q_cross(1), rope_cross(1)):
        d.wait_recv()
    for d in (q_forward(1), rope_forward(1)):
        d.start()
    for d in (q_peer(1), rope_peer(1), rope_peer(2)):
        d.wait_recv()
    rope_forward(1).wait_recv()

    def block(i, final=False):
        a = 2 * i
        done = lax.rem(i + pairs, dummy)
        m, total = softmax(0)
        scores(a + 1, 1)
        finish(i, 0, m, total, values(a, 0))
        combine(done, 0)
        m, total = softmax(1)
        if not final:
            scores(a + 2, 0)
        finish(i, 1, m, total, values(a + 1, 1))
        combine(done, 1)

    def step(i):
        static = isinstance(i, int)
        single = static and i + 1 == pairs
        kv_copy(i + 1).wait()
        q_forward(i + 1, single).wait_recv()
        if static and i == 3:
            rope_forward(2).wait_recv()
        if not static or i + 3 <= pairs:
            kv_copy(i + 3).start()
        if not static or i >= 1:
            for d in o_peer(i - 1):
                d.start()
        if static and i + 1 == pairs:
            o_cross(whole).start()
        if not static:
            @pl.when(lax.rem(i, 4) == 2)
            def _():
                lse_cross((i - 6) // 4).start()

            @pl.when(lax.rem(i, 2) == 0)
            def _():
                o_cross((i - 4) // 2).start()
        elif i >= 4 and i % 2 == 0:
            if i % 4 == 2:
                lse_cross((i - 6) // 4).start()
            o_cross((i - 4) // 2).start()
        if not static or i + 2 <= pairs:
            single = static and i + 2 == pairs
            q_cross(i + 2, single).wait_recv()
            q_forward(i + 2, single).start()
        if static and i == 2:
            rope_cross(2).wait_recv()
            rope_forward(2).start()
        if not static or i >= 2:
            for d in o_peer(i - 2):
                d.wait_recv()
        block(i, static and i == pairs - 1)

    def body(i, c):
        step(i)
        return c

    for i in range(4):
        step(i)
    lax.fori_loop(4, pairs - 3, body, 0)
    for i in range(pairs - 3, pairs):
        step(i)
    i = pairs - 1
    for d in o_peer(i):
        d.start()
    lse_cross(whole // 2).start()
    o_cross(whole + 1).start()
    for j in (i - 1, i):
        for d in o_peer(j):
            d.wait_recv()
        for par in range(2):
            combine(j, par)
        if j == i:
            lse_cross(whole // 2 + 1).start()
        o_cross(j - whole).start()

    def drain_q(k, c):
        q_cross(k).wait_send()
        q_forward(k).wait_send()
        return c

    lax.fori_loop(1, pairs, drain_q, 0)
    for k in (0, pairs):
        q_cross(k, True).wait_send()
        q_forward(k, True).wait_send()
    for k in range(2):
        q_peer(k).wait_send()
    for k in range(3):
        for d in (rope_cross(k), rope_peer(k), rope_forward(k)):
            d.wait_send()

    def drain_peer(k, c):
        for d in o_peer(k):
            d.wait_send()
        return c

    lax.fori_loop(0, pairs, drain_peer, 0)

    def final(g, parts):
        cols = []
        for u in range(2):
            i = 2 * g + u
            l1 = jnp.concatenate([fl[i, 0:1, :32], fl[i, 1:2, :32]], 1)
            l2 = cq[g][:, 64 * u:64 * u + 64]
            top = jnp.maximum(l1, l2)
            e1, e2 = jnp.exp2(l1 - top), jnp.exp2(l2 - top)
            den = e1 + e2
            col = jnp.broadcast_to(jnp.concatenate([e1 / den, e2 / den], 1), (128, 128)).T
            for par in range(2):
                fc[i, par] = fc[i, par] * jnp.concatenate([col[32 * par:32 * par + 32]] * 4, 1)
            cols.append(col[64:])
        for u in range(2):
            i = 2 * g + u
            if u < len(parts):
                parts[u].wait_recv()
            for par in range(2):
                c2 = jnp.concatenate([cols[u][32 * par:32 * par + 32]] * 4, 1)
                o_ref[2 * i + par] = (fc[i, par] + c2 * cr[i, par].astype(F32)).astype(BF).reshape(2, 16, LATENT)

    def final_loop(k, c):
        lse_cross(k).wait()
        for h in range(2):
            final(2 * k + h, (o_cross(2 * k + h),))
        for h in range(2):
            o_cross(2 * k + h).wait_send()
        return c

    lax.fori_loop(0, whole // 2, final_loop, 0)
    for h in range(2):
        lse_cross(whole // 2 + h).wait_recv()
        final(whole + h, (o_cross(whole + 2 * h), o_cross(whole + 2 * h + 1)))
    for h in range(2):
        lse_cross(whole // 2 + h).wait_send()
    for h in range(4):
        o_cross(whole + h).wait_send()


def solution(mesh):
    def local_step(q_blk, kv_blk, len_blk):
        batch, toks, heads, width = q_blk.shape
        pairs = batch // 2
        n = pairs + 2
        vm = pltpu.VMEM
        q_shape = (batch, toks, heads, LATENT)
        rope_shape = (batch, heads, toks * ROPE)
        dma = pltpu.SemaphoreType.DMA
        return pl.pallas_call(
            functools.partial(kernel, batch),
            out_shape=jax.ShapeDtypeStruct(q_shape, BF),
            in_specs=[pl.BlockSpec(memory_space=pltpu.HBM), pl.BlockSpec(memory_space=pltpu.HBM),
                      pl.BlockSpec(memory_space=pltpu.HBM)],
            out_specs=pl.BlockSpec(memory_space=pltpu.VMEM),
            scratch_shapes=[
                pltpu.SMEM((batch,), jnp.int32),
                vm((KV_SLOTS, kv_blk.shape[1], PAGE, width), BF),
                vm((batch, toks, heads, width), BF), vm(q_shape, BF), vm(q_shape, BF), vm(q_shape, BF),
                vm(rope_shape, BF), vm(rope_shape, BF), vm(rope_shape, BF), vm(rope_shape, BF),
                vm((2048, 128), F32), vm((2048, 128), F32), vm((8, 128), F32), vm((8, 128), F32),
                vm((16, 128, 128), BF), vm((16, 128, 128), BF),
                vm((n, 2, 64, LATENT), BF), vm((n, 2, 64, LATENT), BF), vm((n, 2, 64, LATENT), BF),
                vm((n, 2, 128), F32), vm((n, 2, 128), F32), vm((n, 2, 128), F32),
                vm((n, 2, 32, LATENT), BF), vm((n // 2, 1, 128), F32), vm((n, 2, 32, LATENT), BF), vm((n // 2, 1, 128), F32),
                vm((n, 2, 32, LATENT), F32), vm((n, 2, 128), F32),
                dma((KV_SLOTS // 2,)), dma((3,)),
                dma((pairs + 1,)), dma((pairs + 1,)), dma((pairs + 1,)), dma((pairs + 1,)), dma((2,)), dma((2,)),
                dma((9,)), dma((9,)), dma((2, pairs)), dma((2, pairs)), dma((10,)), dma((10,)), dma((5,)), dma((5,)),
            ],
            compiler_params=pltpu.CompilerParams(collective_id=0, has_side_effects=True, vmem_limit_bytes=55_000_000),
        )(*(pltpu.with_memory_space_constraint(x, pltpu.HBM) for x in (q_blk, kv_blk, len_blk)))

    return jax.shard_map(local_step, mesh=mesh, in_specs=(P('dp', None, 'dcp', None), P('dp', None, 'dcp', None, None), P('dp')),
                         out_specs=P('dp', None, 'dcp', None), check_vma=False)
```
